32 devices in a mesh: dp: 1 (over z), u: 4 (over y), r: 8 (over x, core).
Axes of the slice: x: 4, y: 4, z: 1, core: 2. Of those that a mesh axis runs over, the one named last changes fastest.
The devices are a block of a 4x4x8 slice.
Arguments:
- image: bfloat16 [8, 2048, 1536], P('dp', ('r', 'u'))
- text: bfloat16 [8, 160, 1536], P('dp', ('r', 'u'))
- cond_vec: bfloat16 [8, 1536], P('dp')
- key_valid: int32 [8, 160], P('dp')
- w_mod: bfloat16 [2, 2, 1536, 9216], replicated
- b_mod: bfloat16 [2, 2, 9216], replicated
- w_qkv: bfloat16 [2, 2, 1536, 4608], replicated
- b_qkv: bfloat16 [2, 2, 4608], replicated
- q_gain: bfloat16 [2, 2, 24, 64], replicated
- k_gain: bfloat16 [2, 2, 24, 64], replicated
- w_proj: bfloat16 [2, 2, 1536, 1536], replicated
- b_proj: bfloat16 [2, 2, 1536], replicated
- w_up: bfloat16 [2, 2, 1536, 6144], replicated
- b_up: bfloat16 [2, 2, 6144], replicated
- w_down: bfloat16 [2, 2, 6144, 1536], replicated
- b_down: bfloat16 [2, 2, 1536], replicated
Outputs:
- output 1: bfloat16 [8, 2048, 1536], P('dp', ('r', 'u'))
- output 2: bfloat16 [8, 160, 1536], P('dp', ('r', 'u'))
All inputs are finite; a program needn't handle non-finite values.
Results may differ from the reference program's by a relative error of at most 0.0131662.
Values are sent between devices in bfloat16 or wider.
A program may use at most 768 MiB of HBM per device.

```python
import jax
import jax.numpy as jnp
from jax import lax

BATCH = 8
IMG_LEN = 2048
TXT_LEN = 160
CTX_LEN = 154
D_MODEL = 1536
HEADS = 24
HEAD_DIM = 64
MLP_DIM = 6144
BLOCKS = 2

QUERY_BLOCK = min(IMG_LEN, 512)
EPSILON = 1e-6
MASK_FILL = -1e30


def dense_weight(key, shape, fan_in):
    return (jax.random.normal(key, shape, jnp.float32) * fan_in ** -0.5).astype(jnp.bfloat16)


def small_bias(key, shape, spread):
    return (jax.random.normal(key, shape, jnp.float32) * spread).astype(jnp.bfloat16)


def draw_valid(key):
    len_key, pick_key = jax.random.split(key)
    lengths = jax.random.randint(len_key, (BATCH,), 1, CTX_LEN + 1)
    full_row = jax.random.randint(pick_key, (), 0, BATCH)
    lengths = jnp.where(jnp.arange(BATCH) == full_row, CTX_LEN, lengths)
    return (jnp.arange(TXT_LEN)[None, :] < lengths[:, None]).astype(jnp.int32)


def setup_inputs(seed: int = 0, part: int = 0) -> dict:
    base_key = jax.random.key(seed)
    part_keys = jax.random.split(jax.random.fold_in(base_key, part), 4)
    weight_keys = jax.random.split(base_key, 12)
    gain_shape = (BLOCKS, 2, HEADS, HEAD_DIM)
    text_boost = jnp.array([1.0, 1.3], jnp.float32)[None, :, None, None]
    q_gain = jax.random.uniform(weight_keys[4], gain_shape, jnp.float32, 1.0, 2.2)
    k_gain = jax.random.uniform(weight_keys[5], gain_shape, jnp.float32, 1.0, 2.2) * text_boost
    return {
        'image': jax.random.normal(part_keys[0], (BATCH, IMG_LEN, D_MODEL), jnp.float32).astype(jnp.bfloat16),
        'text': jax.random.normal(part_keys[1], (BATCH, TXT_LEN, D_MODEL), jnp.float32).astype(jnp.bfloat16),
        'cond_vec': jax.random.normal(part_keys[2], (BATCH, D_MODEL), jnp.float32).astype(jnp.bfloat16),
        'key_valid': draw_valid(part_keys[3]),
        'w_mod': dense_weight(weight_keys[0], (BLOCKS, 2, D_MODEL, 6 * D_MODEL), D_MODEL),
        'b_mod': small_bias(weight_keys[1], (BLOCKS, 2, 6 * D_MODEL), 0.5),
        'w_qkv': dense_weight(weight_keys[2], (BLOCKS, 2, D_MODEL, 3 * D_MODEL), D_MODEL),
        'b_qkv': small_bias(weight_keys[3], (BLOCKS, 2, 3 * D_MODEL), 0.3),
        'q_gain': q_gain.astype(jnp.bfloat16),
        'k_gain': k_gain.astype(jnp.bfloat16),
        'w_proj': dense_weight(weight_keys[6], (BLOCKS, 2, D_MODEL, D_MODEL), D_MODEL),
        'b_proj': small_bias(weight_keys[7], (BLOCKS, 2, D_MODEL), 0.3),
        'w_up': dense_weight(weight_keys[8], (BLOCKS, 2, D_MODEL, MLP_DIM), D_MODEL),
        'b_up': small_bias(weight_keys[9], (BLOCKS, 2, MLP_DIM), 0.3),
        'w_down': dense_weight(weight_keys[10], (BLOCKS, 2, MLP_DIM, D_MODEL), MLP_DIM),
        'b_down': small_bias(weight_keys[11], (BLOCKS, 2, D_MODEL), 0.3),
    }


def linear(rows, weight, bias):
    flat = jnp.dot(rows.reshape(-1, rows.shape[-1]), weight, preferred_element_type=jnp.float32)
    return flat.reshape(rows.shape[:-1] + (weight.shape[-1],)) + bias.astype(jnp.float32)


def modulated_norm(hidden, shift, scale):
    wide = hidden.astype(jnp.float32)
    centered = wide - jnp.mean(wide, axis=-1, keepdims=True)
    variance = jnp.mean(centered * centered, axis=-1, keepdims=True)
    return ((1.0 + scale) * (centered * lax.rsqrt(variance + EPSILON)) + shift).astype(jnp.bfloat16)


def head_norm(heads_f32, gain):
    mean_sq = jnp.mean(heads_f32 * heads_f32, axis=-1, keepdims=True)
    return (heads_f32 * lax.rsqrt(mean_sq + EPSILON) * gain.astype(jnp.float32)).astype(jnp.bfloat16)


def modality_qkv(hidden, mod_vecs, w_qkv, b_qkv, q_gain, k_gain):
    normed = modulated_norm(hidden, mod_vecs[:, 0], mod_vecs[:, 1])
    packed = linear(normed, w_qkv, b_qkv).reshape(hidden.shape[0], hidden.shape[1], 3, HEADS, HEAD_DIM)
    return head_norm(packed[:, :, 0], q_gain), head_norm(packed[:, :, 1], k_gain), packed[:, :, 2].astype(jnp.bfloat16)


def attend(query, keys, values, key_bias):
    scores = jnp.dot(query, keys.T, preferred_element_type=jnp.float32) * HEAD_DIM ** -0.5 + key_bias
    attn_prob = jax.nn.softmax(scores, axis=-1).astype(jnp.bfloat16)
    return jnp.dot(attn_prob, values, preferred_element_type=jnp.float32).astype(jnp.bfloat16)


def head_attention(operands):
    text_q, image_q, keys, values, key_bias = operands
    text_out = attend(text_q, keys, values, key_bias)

    def image_block(block_q):
        return attend(block_q, keys, values, key_bias)

    image_out = lax.map(image_block, image_q.reshape(IMG_LEN // QUERY_BLOCK, QUERY_BLOCK, HEAD_DIM))
    return text_out, image_out.reshape(IMG_LEN, HEAD_DIM)


def by_head(heads_arr):
    return heads_arr.transpose(0, 2, 1, 3).reshape(-1, heads_arr.shape[1], HEAD_DIM)


def from_head(flat):
    return flat.reshape(BATCH, HEADS, -1, HEAD_DIM).transpose(0, 2, 1, 3).reshape(BATCH, -1, D_MODEL)


def joint_attention(text_qkv, image_qkv, key_valid):
    keys = jnp.concatenate([text_qkv[1], image_qkv[1]], axis=1)
    values = jnp.concatenate([text_qkv[2], image_qkv[2]], axis=1)
    text_bias = jnp.where(key_valid > 0, 0.0, MASK_FILL).astype(jnp.float32)
    key_bias = jnp.concatenate([text_bias, jnp.zeros((BATCH, IMG_LEN), jnp.float32)], axis=1)
    text_out, image_out = lax.map(head_attention, (by_head(text_qkv[0]), by_head(image_qkv[0]), by_head(keys), by_head(values), jnp.repeat(key_bias, HEADS, axis=0)))
    return from_head(text_out), from_head(image_out)


def modality_out(hidden, attended, mod_vecs, w_proj, b_proj, w_up, b_up, w_down, b_down):
    residual = hidden.astype(jnp.float32) + mod_vecs[:, 2] * linear(attended, w_proj, b_proj)
    hidden = residual.astype(jnp.bfloat16)
    normed = modulated_norm(hidden, mod_vecs[:, 3], mod_vecs[:, 4])
    inner = jax.nn.gelu(linear(normed, w_up, b_up), approximate=True).astype(jnp.bfloat16)
    return (hidden.astype(jnp.float32) + mod_vecs[:, 5] * linear(inner, w_down, b_down)).astype(jnp.bfloat16)


def reference(image, text, cond_vec, key_valid, w_mod, b_mod, w_qkv, b_qkv, q_gain, k_gain, w_proj, b_proj, w_up, b_up, w_down, b_down):
    silu_vec = jax.nn.silu(cond_vec.astype(jnp.float32)).astype(jnp.bfloat16)
    for block in range(BLOCKS):
        sides = [image, text]
        mod_list = [linear(silu_vec, w_mod[block, side], b_mod[block, side]).reshape(BATCH, 6, 1, D_MODEL) for side in range(2)]
        projected = [modality_qkv(sides[side], mod_list[side], w_qkv[block, side], b_qkv[block, side], q_gain[block, side], k_gain[block, side]) for side in range(2)]
        text_att, image_att = joint_attention(projected[1], projected[0], key_valid)
        attended = [image_att, text_att]
        image, text = [modality_out(sides[side], attended[side], mod_list[side], w_proj[block, side], b_proj[block, side], w_up[block, side], b_up[block, side], w_down[block, side], b_down[block, side]) for side in range(2)]
    return image, text
```

```python
import functools
import math

import jax
import jax.numpy as jnp
from jax import lax
from jax.experimental import pallas as pl
from jax.experimental.pallas import tpu as pltpu
from jax.sharding import PartitionSpec as P

EPSILON = 1e-6
MASK_FILL = -1e30
MESH = pl.DeviceIdType.MESH
VMEM = pltpu.VMEM
LANES = 128
TXT_PAD = 48
Q_BLOCK = 256


def place():
    r, u = lax.axis_index('r'), lax.axis_index('u')
    return r, u, r % 2, r // 2


def pick(c, even, odd):
    return (1 - c) * even + c * odd


def remote(src, dst, send, recv, r, u):
    return pltpu.make_async_remote_copy(src_ref=src, dst_ref=dst, send_sem=send, recv_sem=recv, device_id={'r': r, 'u': u}, device_id_type=MESH)


def greet(peers, count):
    barrier = pltpu.get_barrier_semaphore()
    for r, u in peers:
        pl.semaphore_signal(barrier, inc=1, device_id={'r': r, 'u': u}, device_id_type=MESH)
    pl.semaphore_wait(barrier, count)


def scatter_kernel(n, img, txt, mod, img_o, txt_o, mod_o, send, recv, mod_send, mod_recv, local):
    r, u, c, x = place()
    total = 2 * n * n
    me = r * n + u
    others = [(me + d) % total for d in range(1, total)]
    greet([(o // n, o % n) for o in others], total - 1)
    copies = []
    for d, o in enumerate(others):
        ro, uo = o // n, o % n
        sample = pick(ro % 2, uo, n + ro // 2)
        copies.append(remote(mod.at[sample], mod_o.at[me], mod_send.at[d], mod_recv.at[d], ro, uo))
    own_slot = pick(c, u, r)
    targets = []
    for d in list(range(1, n)):
        targets.append((pick(c, r, 2 * ((x + d) % n) + 1), pick(c, (u + d) % n, u), pick(c, (u + d) % n, n + (x + d) % n), own_slot))
    for d in range(n):
        j = (pick(c, x, u) + d) % n
        targets.append((pick(c, 2 * j + 1, 2 * x), pick(c, u, j), pick(c, n + j, j), pick(c, r, n + u)))
    for t, (ro, uo, sample, slot) in enumerate(targets):
        copies.append(remote(img.at[sample], img_o.at[slot], send.at[0, t], recv.at[0, slot], ro, uo))
        copies.append(remote(txt.at[sample], txt_o.at[slot], send.at[1, t], recv.at[1, slot], ro, uo))
    for copy in copies:
        copy.start()
    own_sample = pick(c, u, n + x)
    mine = [
        pltpu.make_async_copy(img.at[own_sample], img_o.at[own_slot], local.at[0]),
        pltpu.make_async_copy(txt.at[own_sample], txt_o.at[own_slot], local.at[1]),
        pltpu.make_async_copy(mod.at[own_sample], mod_o.at[me], local.at[2]),
    ]
    for copy in mine:
        copy.start()
    for copy in copies:
        copy.wait_send()
    for copy in mine:
        copy.wait()
    for d in range(1, total):
        source = (me - d + total) % total
        remote(mod.at[0], mod_o.at[source], mod_send.at[d - 1], mod_recv.at[d - 1], r, u).wait_recv()
    for d in range(1, 2 * n):
        slot = (own_slot + d) % (2 * n)
        remote(img.at[0], img_o.at[slot], send.at[0, 0], recv.at[0, slot], r, u).wait_recv()
        remote(txt.at[0], txt_o.at[slot], send.at[1, 0], recv.at[1, slot], r, u).wait_recv()


def scatter(mesh, img, txt, mod):
    n = mesh.shape['u']
    total = 2 * n * n
    return pl.pallas_call(
        functools.partial(scatter_kernel, n),
        out_shape=[jax.ShapeDtypeStruct(img.shape, img.dtype), jax.ShapeDtypeStruct(txt.shape, txt.dtype), jax.ShapeDtypeStruct((total,) + mod.shape[1:], mod.dtype)],
        in_specs=[pl.BlockSpec(memory_space=VMEM)] * 3,
        out_specs=[pl.BlockSpec(memory_space=VMEM)] * 3,
        scratch_shapes=[pltpu.SemaphoreType.DMA((2, 2 * n)), pltpu.SemaphoreType.DMA((2, 2 * n)), pltpu.SemaphoreType.DMA((total,)), pltpu.SemaphoreType.DMA((total,)), pltpu.SemaphoreType.DMA((3,))],
        compiler_params=pltpu.CompilerParams(collective_id=0, has_side_effects=True),
        name='scatter',
    )(img, txt, mod)


def unscatter_kernel(n, img, txt, img_o, txt_o, send, recv, local):
    r, u, c, x = place()
    own_slot, sample = pick(c, u, r), pick(c, u, n + x)
    senders, targets = [], []
    for d in range(1, 2 * n):
        s = (sample + d) % (2 * n)
        odd = s // n
        senders.append((pick(odd, 2 * x, 2 * (s % n) + 1), pick(odd, s, u)))
        k = (own_slot + d) % (2 * n)
        targets.append((pick(c, 2 * x + k // n, k), pick(c, k % n, u), k))
    greet(senders, 2 * n - 1)
    copies = []
    for t, (ro, uo, k) in enumerate(targets):
        copies.append(remote(img.at[k], img_o.at[sample], send.at[0, t], recv.at[0, sample], ro, uo))
        copies.append(remote(txt.at[k], txt_o.at[sample], send.at[1, t], recv.at[1, sample], ro, uo))
    for copy in copies:
        copy.start()
    mine = [pltpu.make_async_copy(img.at[own_slot], img_o.at[sample], local.at[0]), pltpu.make_async_copy(txt.at[own_slot], txt_o.at[sample], local.at[1])]
    for copy in mine:
        copy.start()
    for copy in copies:
        copy.wait_send()
    for copy in mine:
        copy.wait()
    for d in range(1, 2 * n):
        s = (sample + d) % (2 * n)
        remote(img.at[0], img_o.at[s], send.at[0, 0], recv.at[0, s], r, u).wait_recv()
        remote(txt.at[0], txt_o.at[s], send.at[1, 0], recv.at[1, s], r, u).wait_recv()


def unscatter(mesh, img, txt):
    n = mesh.shape['u']
    return pl.pallas_call(
        functools.partial(unscatter_kernel, n),
        out_shape=[jax.ShapeDtypeStruct(img.shape, img.dtype), jax.ShapeDtypeStruct(txt.shape, txt.dtype)],
        in_specs=[pl.BlockSpec(memory_space=VMEM)] * 2,
        out_specs=[pl.BlockSpec(memory_space=VMEM)] * 2,
        scratch_shapes=[pltpu.SemaphoreType.DMA((2, 2 * n)), pltpu.SemaphoreType.DMA((2, 2 * n)), pltpu.SemaphoreType.DMA((2,))],
        compiler_params=pltpu.CompilerParams(collective_id=1, has_side_effects=True),
        name='unscatter',
    )(img, txt)


def ring_place(n):
    r, u, c, x = place()
    me = pick(c, x, u)

    def peer(d):
        j = (me + d + n) % n
        return pick(c, 2 * j, r), pick(c, u, j)

    return me, peer


def gather_kernel(n, img, txt, img_o, txt_o, send, recv, local):
    me, peer = ring_place(n)
    right, left = peer(1), peer(-1)
    greet([right, left], 2)
    rows = img.shape[0] // 4
    lside, rside, far = (me + n - 1) % n, (me + 1) % n, (me + 2) % n

    def part(ref, txt_ref, q):
        return txt_ref if q == 4 else ref.at[pl.ds(q * rows, rows)]

    def block(slot, q):
        return part(img_o.at[slot], txt_o.at[slot], q)

    copies = []
    for q_right, q_left in zip((0, 1, 4, 2, 3), (2, 3, 4, 0, 1)):
        copies.append(remote(part(img, txt, q_right), block(me, q_right), send.at[0, q_right], recv.at[0, q_right], *right))
        copies.append(remote(part(img, txt, q_left), block(me, q_left), send.at[1, q_left], recv.at[1, q_left], *left))
    for copy in copies:
        copy.start()
    mine = [pltpu.make_async_copy(img, img_o.at[me], local.at[0]), pltpu.make_async_copy(txt, txt_o.at[me], local.at[1])]
    for copy in mine:
        copy.start()

    def arrived(kind, slot, q):
        remote(block(slot, q), block(slot, q), send.at[0, q], recv.at[kind, q], *right).wait_recv()

    for kind, slot, q, target in ((0, lside, 0, right), (1, rside, 2, left), (0, lside, 1, right), (1, rside, 3, left), (0, lside, 4, right)):
        arrived(kind, slot, q)
        copy = remote(block(slot, q), block(slot, q), send.at[2, q], recv.at[2, q], *target)
        copy.start()
        copies.append(copy)
    for kind, slot, parts in ((0, lside, (2, 3)), (1, rside, (4, 0, 1)), (2, far, (0, 2, 1, 3, 4))):
        for q in parts:
            arrived(kind, slot, q)
    for copy in copies:
        copy.wait_send()
    for copy in mine:
        copy.wait()


def gather(mesh, img, txt, collective_id):
    n = mesh.shape['u']
    return pl.pallas_call(
        functools.partial(gather_kernel, n),
        out_shape=[jax.ShapeDtypeStruct((n,) + img.shape, img.dtype), jax.ShapeDtypeStruct((n,) + txt.shape, txt.dtype)],
        in_specs=[pl.BlockSpec(memory_space=VMEM)] * 2,
        out_specs=[pl.BlockSpec(memory_space=VMEM)] * 2,
        scratch_shapes=[pltpu.SemaphoreType.DMA((3, 5)), pltpu.SemaphoreType.DMA((3, 5)), pltpu.SemaphoreType.DMA((2,))],
        compiler_params=pltpu.CompilerParams(collective_id=collective_id, has_side_effects=True),
        name='gather',
    )(img, txt)


def exchange_kernel(n, o, img_o, txt_o, send, recv, local):
    me, peer = ring_place(n)
    greet([peer(d) for d in range(1, n)], n - 1)
    rows, cols = img_o.shape[0], o.shape[1]
    txt_rows = txt_o.shape[0]

    def sources(member):
        return o.at[pl.ds(pl.multiple_of(member * rows, rows), rows)], o.at[pl.ds(pl.multiple_of(n * rows + member * txt_rows, 16), txt_rows)]

    def targets(member):
        span = pl.ds(pl.multiple_of(member * cols, LANES), cols)
        return img_o.at[:, span], txt_o.at[:, span]

    copies = []
    for d in (2, 1, 3):
        for t, (src, dst) in enumerate(zip(sources((me + d) % n), targets(me))):
            copies.append(remote(src, dst, send.at[t, d - 1], recv.at[t, d - 1], *peer(d)))
    for copy in copies:
        copy.start()
    mine = [pltpu.make_async_copy(src, dst, local.at[t]) for t, (src, dst) in enumerate(zip(sources(me), targets(me)))]
    for copy in mine:
        copy.start()
    for copy in copies:
        copy.wait_send()
    for copy in mine:
        copy.wait()
    for d in range(1, n):
        for t, (src, dst) in enumerate(zip(sources(me), targets((me + n - d) % n))):
            remote(src, dst, send.at[t, d - 1], recv.at[t, d - 1], *peer(1)).wait_recv()


def exchange(mesh, o, img_rows, txt_rows, collective_id):
    n = mesh.shape['u']
    return pl.pallas_call(
        functools.partial(exchange_kernel, n),
        out_shape=[jax.ShapeDtypeStruct((img_rows, n * o.shape[1]), o.dtype), jax.ShapeDtypeStruct((txt_rows, n * o.shape[1]), o.dtype)],
        in_specs=[pl.BlockSpec(memory_space=VMEM)],
        out_specs=[pl.BlockSpec(memory_space=VMEM)] * 2,
        scratch_shapes=[pltpu.SemaphoreType.DMA((2, n)), pltpu.SemaphoreType.DMA((2, n)), pltpu.SemaphoreType.DMA((2,))],
        compiler_params=pltpu.CompilerParams(collective_id=collective_id, has_side_effects=True),
        name='exchange',
    )(o)


def attend_kernel(head_dim, me_ref, a_img, a_txt, wq_i, wk_i, wv_i, wq_t, wk_t, wv_t, bias_i, bias_t, gain_i, gain_t, key_bias, o_ref, w_cat, q_s, k_s, v_s):
    img_rows, txt_rows = a_img.shape[0], a_txt.shape[0]
    low = lax.broadcasted_iota(jnp.int32, (Q_BLOCK, LANES), 1) < head_dim

    def unit(part, gain):
        square = part * part
        mask = low[: part.shape[0]]
        first = jnp.sum(jnp.where(mask, square, 0.0), axis=-1, keepdims=True)
        second = jnp.sum(jnp.where(mask, 0.0, square), axis=-1, keepdims=True)
        scale = lax.rsqrt(jnp.where(mask, first, second) * (1.0 / head_dim) + EPSILON)
        return (part * scale * gain).astype(jnp.bfloat16)

    def project(rows, bias, gain, out_rows):
        packed = jnp.dot(rows, w_cat[...], preferred_element_type=jnp.float32) + bias[0]
        q_s[out_rows, :] = unit(packed[:, :LANES], gain[0, :, :LANES])
        k_s[out_rows, :] = unit(packed[:, LANES:2 * LANES], gain[0, :, LANES:])
        v_s[out_rows, :] = packed[:, 2 * LANES:].astype(jnp.bfloat16)

    for t, w in enumerate((wq_t, wk_t, wv_t)):
        w_cat[:, t * LANES:(t + 1) * LANES] = w[0, 0]
    project(a_txt[...], bias_t, gain_t, pl.ds(img_rows, txt_rows))
    tail = pl.ds(img_rows + txt_rows, q_s.shape[0] - img_rows - txt_rows)
    for ref in (q_s, k_s, v_s):
        ref[tail, :] = jnp.zeros((q_s.shape[0] - img_rows - txt_rows, LANES), jnp.bfloat16)
    for t, w in enumerate((wq_i, wk_i, wv_i)):
        w_cat[:, t * LANES:(t + 1) * LANES] = w[0, 0]

    @pl.loop(0, img_rows // Q_BLOCK)
    def _(step):
        span = pl.ds(pl.multiple_of(step * Q_BLOCK, Q_BLOCK), Q_BLOCK)
        project(a_img[span, :], bias_i, gain_i, span)

    factor = math.log2(math.e) / math.sqrt(head_dim)

    @pl.loop(0, q_s.shape[0] // Q_BLOCK)
    def _(step):
        span = pl.ds(pl.multiple_of(step * Q_BLOCK, Q_BLOCK), Q_BLOCK)
        query = q_s[span, :]
        zero = jnp.zeros_like(query)
        keys, values = k_s[...], v_s[...]
        halves = []
        for h in range(2):
            one = jnp.where(low, query, zero) if h == 0 else jnp.where(low, zero, query)
            scores = lax.dot_general(one, keys, (((1,), (1,)), ((), ())), preferred_element_type=jnp.float32)
            scores = jnp.concatenate([scores[:, :img_rows], scores[:, img_rows:] + key_bias[...]], axis=1)
            top = jnp.max(scores, axis=-1, keepdims=True)
            prob = jnp.exp2((scores - top) * factor)
            norm = jnp.sum(prob, axis=-1, keepdims=True)
            halves.append(jnp.dot(prob.astype(jnp.bfloat16), values, preferred_element_type=jnp.float32) / norm)
        o_ref[span, :] = jnp.where(low, halves[0], halves[1]).astype(jnp.bfloat16)


def attend(me, a_img, a_txt, w_qkv, bias, gain, key_bias, block, head_dim):
    n, img_rows, width = a_img.shape
    a_img = a_img.reshape(-1, width)
    a_txt = a_txt.reshape(-1, width)
    rows = a_img.shape[0] + Q_BLOCK
    cols = width // n
    pairs = cols // LANES
    third = width // LANES

    def weight(side, t):
        return pl.BlockSpec((1, 1, width, LANES), lambda p, me_ref: (block, side, 0, t * third + me_ref[0] * pairs + p))

    whole = lambda shape: pl.BlockSpec(shape, lambda p, me_ref: (0,) * len(shape))
    vec = lambda side, size: pl.BlockSpec((1, 1, size), lambda p, me_ref: (side * pairs + p, 0, 0))
    return pl.pallas_call(
        functools.partial(attend_kernel, head_dim),
        out_shape=jax.ShapeDtypeStruct((rows, cols), jnp.bfloat16),
        grid_spec=pltpu.PrefetchScalarGridSpec(
            num_scalar_prefetch=1,
            grid=(pairs,),
            in_specs=[whole(a_img.shape), whole(a_txt.shape)] + [weight(s, t) for s in range(2) for t in range(3)] + [vec(0, 3 * LANES), vec(1, 3 * LANES), vec(0, 2 * LANES), vec(1, 2 * LANES), whole(key_bias.shape)],
            out_specs=pl.BlockSpec((rows, LANES), lambda p, me_ref: (0, p)),
            scratch_shapes=[pltpu.VMEM((width, 3 * LANES), jnp.bfloat16)] + [pltpu.VMEM((rows, LANES), jnp.bfloat16)] * 3,
        ),
        compiler_params=pltpu.CompilerParams(vmem_limit_bytes=60 * 2**20, dimension_semantics=('arbitrary',)),
        cost_estimate=pl.CostEstimate(flops=10**10, bytes_accessed=10**7, transcendentals=0),
        name='attend',
    )(me, a_img, a_txt, w_qkv, w_qkv, w_qkv, w_qkv, w_qkv, w_qkv, bias, bias, gain, gain, key_bias)


def modulated_norm(hidden, shift, scale):
    wide = hidden.astype(jnp.float32)
    centered = wide - jnp.mean(wide, axis=-1, keepdims=True)
    variance = jnp.mean(centered * centered, axis=-1, keepdims=True)
    return ((1.0 + scale) * (centered * lax.rsqrt(variance + EPSILON)) + shift).astype(jnp.bfloat16)


def linear(rows, weight, bias):
    return jnp.dot(rows, weight, preferred_element_type=jnp.float32) + bias.astype(jnp.float32)


def modality_out(hidden, attended, mod, w_proj, b_proj, w_up, b_up, w_down, b_down):
    residual = hidden.astype(jnp.float32) + mod[2] * linear(attended, w_proj, b_proj)
    hidden = residual.astype(jnp.bfloat16)
    normed = modulated_norm(hidden, mod[3], mod[4])
    inner = jax.nn.gelu(linear(normed, w_up, b_up), approximate=True).astype(jnp.bfloat16)
    return (hidden.astype(jnp.float32) + mod[5] * linear(inner, w_down, b_down)).astype(jnp.bfloat16)


def solution(mesh):
    seq_spec = P('dp', ('r', 'u'), None)
    row_spec = P('dp', None)
    n = mesh.shape['u']
    total = n * mesh.shape['r']

    def local_blocks(image, text, cond_vec, key_valid, w_mod, b_mod, w_qkv, b_qkv, q_gain, k_gain, w_proj, b_proj, w_up, b_up, w_down, b_down):
        blocks, _, width, mod_width = w_mod.shape
        heads, head_dim = q_gain.shape[2:]
        r, u = lax.axis_index('r'), lax.axis_index('u')
        c, x = r % 2, r // 2
        sample = jnp.where(c == 0, u, n + x)
        member = jnp.where(c == 0, x, u)
        silu_vec = jax.nn.silu(cond_vec.astype(jnp.float32)).astype(jnp.bfloat16)
        per = blocks * 2 * mod_width // total
        parts = mod_width // per
        me = r * n + u
        which, col = me // parts, (me % parts) * per
        w_mine = lax.dynamic_slice(w_mod, (which // 2, which % 2, 0, col), (1, 1, width, per))[0, 0]
        b_mine = lax.dynamic_slice(b_mod, (which // 2, which % 2, col), (1, 1, per))[0, 0]
        mod_mine = jnp.dot(silu_vec, w_mine, preferred_element_type=jnp.float32) + b_mine.astype(jnp.float32)
        img, txt, mod_all = scatter(mesh, image, text, mod_mine.reshape(-1, per // LANES, LANES))
        mod_all = mod_all.reshape(blocks, 2, 6, 1, width)
        slots, run, _ = img.shape
        txt_run = txt.shape[1]
        img = img.reshape(slots * run, width)
        txt = jnp.pad(txt.reshape(slots * txt_run, width), ((0, TXT_PAD - slots * txt_run), (0, 0)))

        valid = lax.dynamic_slice(key_valid, (sample, 0), (1, key_valid.shape[1]))[0]
        strided = valid.reshape(2 * n, n, txt_run).transpose(1, 0, 2).reshape(-1)
        valid = jnp.where(c == 0, valid, strided).reshape(n, slots * txt_run)
        text_bias = jnp.pad(jnp.where(valid > 0, 0.0, MASK_FILL), ((0, 0), (0, TXT_PAD - slots * txt_run)), constant_values=MASK_FILL).reshape(1, -1)
        key_bias = jnp.pad(text_bias, ((0, 0), (0, Q_BLOCK - n * TXT_PAD)), constant_values=MASK_FILL).astype(jnp.float32)

        pairs = width // n // LANES
        bias_all = b_qkv.astype(jnp.float32).reshape(blocks, 2, 3, n, pairs, LANES)
        bias_all = lax.dynamic_index_in_dim(bias_all, member, 3, keepdims=False).transpose(0, 1, 3, 2, 4).reshape(blocks, 2 * pairs, 1, 3 * LANES)
        gain_all = jnp.stack([q_gain, k_gain], axis=2).astype(jnp.float32).reshape(blocks, 2, 2, n, pairs, LANES)
        gain_all = lax.dynamic_index_in_dim(gain_all, member, 3, keepdims=False).transpose(0, 1, 3, 2, 4).reshape(blocks, 2 * pairs, 1, 2 * LANES)
        member_arr = member.reshape(1).astype(jnp.int32)

        sides = [img, txt]
        for block in range(blocks):
            normed = [modulated_norm(sides[s], mod_all[block, s, 0], mod_all[block, s, 1]) for s in range(2)]
            a_img, a_txt = gather(mesh, normed[0], normed[1], 2 + 2 * block)
            o = attend(member_arr, a_img, a_txt, w_qkv, bias_all[block], gain_all[block], key_bias, block, head_dim)
            attended = exchange(mesh, o, img.shape[0], TXT_PAD, 3 + 2 * block)
            sides = [modality_out(sides[s], attended[s], mod_all[block, s], w_proj[block, s], b_proj[block, s], w_up[block, s], b_up[block, s], w_down[block, s], b_down[block, s]) for s in range(2)]
        img = sides[0].reshape(slots, run, width)
        txt = sides[1][: slots * txt_run].reshape(slots, txt_run, width)
        return unscatter(mesh, img, txt)

    return jax.shard_map(local_blocks, mesh=mesh, in_specs=(seq_spec, seq_spec, row_spec, row_spec) + (P(),) * 12, out_specs=(seq_spec, seq_spec), check_vma=False)
```

```python
import functools
import math

import jax
import jax.numpy as jnp
from jax import lax
from jax.experimental import pallas as pl
from jax.experimental.pallas import tpu as pltpu
from jax.sharding import PartitionSpec as P

EPSILON = 1e-6
MASK_FILL = -1e30
MESH = pl.DeviceIdType.MESH
VMEM = pltpu.VMEM
LANES = 128
TXT_PAD = 48
TXT_ROWS = 256
Q_BLOCK = 768
K_BLOCK = 256


def place():
    r, u = lax.axis_index('r'), lax.axis_index('u')
    return r, u, r % 2, r // 2


def pick(c, even, odd):
    return (1 - c) * even + c * odd


def remote(src, dst, send, recv, r, u):
    return pltpu.make_async_remote_copy(src_ref=src, dst_ref=dst, send_sem=send, recv_sem=recv, device_id={'r': r, 'u': u}, device_id_type=MESH)


def greet(peers, count):
    barrier = pltpu.get_barrier_semaphore()
    for r, u in peers:
        pl.semaphore_signal(barrier, inc=1, device_id={'r': r, 'u': u}, device_id_type=MESH)
    pl.semaphore_wait(barrier, count)


def scatter_kernel(n, img, txt, mod, img_o, txt_o, mod_o, send, recv, mod_send, mod_recv, local):
    r, u, c, x = place()
    total = 2 * n * n
    me = r * n + u
    others = [(me + d) % total for d in range(1, total)]
    greet([(o // n, o % n) for o in others], total - 1)
    copies = []
    for d, o in enumerate(others):
        ro, uo = o // n, o % n
        sample = pick(ro % 2, uo, n + ro // 2)
        copies.append(remote(mod.at[sample], mod_o.at[me], mod_send.at[d], mod_recv.at[d], ro, uo))
    own_slot = pick(c, u, r)
    targets = []
    for d in list(range(1, n)):
        targets.append((pick(c, r, 2 * ((x + d) % n) + 1), pick(c, (u + d) % n, u), pick(c, (u + d) % n, n + (x + d) % n), own_slot))
    for d in range(n):
        j = (pick(c, x, u) + d) % n
        targets.append((pick(c, 2 * j + 1, 2 * x), pick(c, u, j), pick(c, n + j, j), pick(c, r, n + u)))
    for t, (ro, uo, sample, slot) in enumerate(targets):
        copies.append(remote(img.at[sample], img_o.at[slot], send.at[0, t], recv.at[0, slot], ro, uo))
        copies.append(remote(txt.at[sample], txt_o.at[slot], send.at[1, t], recv.at[1, slot], ro, uo))
    for copy in copies:
        copy.start()
    own_sample = pick(c, u, n + x)
    mine = [
        pltpu.make_async_copy(img.at[own_sample], img_o.at[own_slot], local.at[0]),
        pltpu.make_async_copy(txt.at[own_sample], txt_o.at[own_slot], local.at[1]),
        pltpu.make_async_copy(mod.at[own_sample], mod_o.at[me], local.at[2]),
    ]
    for copy in mine:
        copy.start()
    for copy in copies:
        copy.wait_send()
    for copy in mine:
        copy.wait()
    for d in range(1, total):
        source = (me - d + total) % total
        remote(mod.at[0], mod_o.at[source], mod_send.at[d - 1], mod_recv.at[d - 1], r, u).wait_recv()
    for d in range(1, 2 * n):
        slot = (own_slot + d) % (2 * n)
        remote(img.at[0], img_o.at[slot], send.at[0, 0], recv.at[0, slot], r, u).wait_recv()
        remote(txt.at[0], txt_o.at[slot], send.at[1, 0], recv.at[1, slot], r, u).wait_recv()


def scatter(mesh, img, txt, mod):
    n = mesh.shape['u']
    total = 2 * n * n
    return pl.pallas_call(
        functools.partial(scatter_kernel, n),
        out_shape=[jax.ShapeDtypeStruct(img.shape, img.dtype), jax.ShapeDtypeStruct(txt.shape, txt.dtype), jax.ShapeDtypeStruct((total,) + mod.shape[1:], mod.dtype)],
        in_specs=[pl.BlockSpec(memory_space=VMEM)] * 3,
        out_specs=[pl.BlockSpec(memory_space=VMEM)] * 3,
        scratch_shapes=[pltpu.SemaphoreType.DMA((2, 2 * n)), pltpu.SemaphoreType.DMA((2, 2 * n)), pltpu.SemaphoreType.DMA((total,)), pltpu.SemaphoreType.DMA((total,)), pltpu.SemaphoreType.DMA((3,))],
        compiler_params=pltpu.CompilerParams(collective_id=0, has_side_effects=True),
        name='scatter',
    )(img, txt, mod)


def unscatter_kernel(n, img, txt, img_o, txt_o, send, recv, local):
    r, u, c, x = place()
    own_slot, sample = pick(c, u, r), pick(c, u, n + x)
    senders, targets = [], []
    for d in range(1, 2 * n):
        s = (sample + d) % (2 * n)
        odd = s // n
        senders.append((pick(odd, 2 * x, 2 * (s % n) + 1), pick(odd, s, u)))
        k = (own_slot + d) % (2 * n)
        targets.append((pick(c, 2 * x + k // n, k), pick(c, k % n, u), k))
    greet(senders, 2 * n - 1)
    copies = []
    for t, (ro, uo, k) in enumerate(targets):
        copies.append(remote(img.at[k], img_o.at[sample], send.at[0, t], recv.at[0, sample], ro, uo))
        copies.append(remote(txt.at[k], txt_o.at[sample], send.at[1, t], recv.at[1, sample], ro, uo))
    for copy in copies:
        copy.start()
    mine = [pltpu.make_async_copy(img.at[own_slot], img_o.at[sample], local.at[0]), pltpu.make_async_copy(txt.at[own_slot], txt_o.at[sample], local.at[1])]
    for copy in mine:
        copy.start()
    for copy in copies:
        copy.wait_send()
    for copy in mine:
        copy.wait()
    for d in range(1, 2 * n):
        s = (sample + d) % (2 * n)
        remote(img.at[0], img_o.at[s], send.at[0, 0], recv.at[0, s], r, u).wait_recv()
        remote(txt.at[0], txt_o.at[s], send.at[1, 0], recv.at[1, s], r, u).wait_recv()


def unscatter(mesh, img, txt):
    n = mesh.shape['u']
    return pl.pallas_call(
        functools.partial(unscatter_kernel, n),
        out_shape=[jax.ShapeDtypeStruct(img.shape, img.dtype), jax.ShapeDtypeStruct(txt.shape, txt.dtype)],
        in_specs=[pl.BlockSpec(memory_space=VMEM)] * 2,
        out_specs=[pl.BlockSpec(memory_space=VMEM)] * 2,
        scratch_shapes=[pltpu.SemaphoreType.DMA((2, 2 * n)), pltpu.SemaphoreType.DMA((2, 2 * n)), pltpu.SemaphoreType.DMA((2,))],
        compiler_params=pltpu.CompilerParams(collective_id=1, has_side_effects=True),
        name='unscatter',
    )(img, txt)


def ring_place(n):
    r, u, c, x = place()
    me = pick(c, x, u)

    def peer(d):
        j = (me + d + n) % n
        return pick(c, 2 * j, r), pick(c, u, j)

    return me, peer


def joint_kernel(n, head_dim, block, img, txt, w_qkv, bias, gain, key_bias, img_o, txt_o, a_img, a_txt, w_i, w_t, q_s, k_s, v_s, s_a, s_b, o_s, send, recv, o_send, o_recv, local):
    me, peer = ring_place(n)
    right, left = peer(1), peer(-1)
    rows, width = img.shape
    txt_rows = txt.shape[0]
    img_rows = n * rows
    pairs, all_rows = q_s.shape[:2]
    cols = pairs * LANES
    weights = []
    for side, ref in ((0, w_i), (1, w_t)):
        for t in range(3):
            start = pl.multiple_of(t * width + me * cols, LANES)
            weights.append(pltpu.make_async_copy(w_qkv.at[block, side, :, pl.ds(start, cols)], ref.at[:, pl.ds(t * cols, cols)], local.at[2 + 3 * side + t]))
    for copy in weights:
        copy.start()
    mine = [pltpu.make_async_copy(img, a_img.at[me], local.at[0]), pltpu.make_async_copy(txt, a_txt.at[me], local.at[1])]
    for copy in mine:
        copy.start()
    greet([peer(d) for d in range(1, n)], n - 1)
    piece = rows // 4
    lside, rside, far = (me + n - 1) % n, (me + 1) % n, (me + 2) % n

    def part(ref, txt_ref, q):
        return txt_ref if q == 4 else ref.at[pl.ds(q * piece, piece)]

    def landing(slot, q):
        return part(a_img.at[slot], a_txt.at[slot], q)

    copies = []
    for q_right, q_left in zip((0, 1, 4, 2, 3), (2, 3, 4, 0, 1)):
        copies.append(remote(part(img, txt, q_right), landing(me, q_right), send.at[0, q_right], recv.at[0, q_right], *right))
        copies.append(remote(part(img, txt, q_left), landing(me, q_left), send.at[1, q_left], recv.at[1, q_left], *left))
    for copy in copies:
        copy.start()

    def arrived(kind, slot, q):
        remote(landing(slot, q), landing(slot, q), send.at[0, q], recv.at[kind, q], *right).wait_recv()

    def forward(kind, slot, q, target):
        arrived(kind, slot, q)
        copy = remote(landing(slot, q), landing(slot, q), send.at[2, q], recv.at[2, q], *target)
        copy.start()

    low = lax.broadcasted_iota(jnp.int32, (Q_BLOCK, LANES), 1) < head_dim

    def unit(part, scale_by):
        square = part * part
        mask = low[: part.shape[0]]
        first = jnp.sum(jnp.where(mask, square, 0.0), axis=-1, keepdims=True)
        second = jnp.sum(jnp.where(mask, 0.0, square), axis=-1, keepdims=True)
        scale = lax.rsqrt(jnp.where(mask, first, second) * (1.0 / head_dim) + EPSILON)
        return (part * scale * scale_by).astype(jnp.bfloat16)

    def project(tokens, weight, side, spans):
        for tile in range(0, 3 * pairs, 2):
            count = min(2, 3 * pairs - tile)
            lanes = slice(tile * LANES, (tile + count) * LANES)
            packed = jnp.dot(tokens, weight[:, lanes], preferred_element_type=jnp.float32) + bias[side:side + 1, lanes]
            for k in range(count):
                kind, p = (tile + k) // pairs, (tile + k) % pairs
                value = packed[:, k * LANES:(k + 1) * LANES]
                if kind < 2:
                    value = unit(value, gain[side:side + 1, (tile + k) * LANES:(tile + k + 1) * LANES])
                else:
                    value = value.T.astype(jnp.bfloat16)
                offset = 0
                for start, size in spans:
                    if kind == 0:
                        q_s[p, pl.ds(start, size), :] = value[offset:offset + size]
                    elif kind == 1:
                        k_s[p, pl.ds(start, size), :] = value[offset:offset + size]
                    else:
                        v_s[p, :, pl.ds(start, size)] = value[:, offset:offset + size]
                    offset += size

    for copy in weights + mine:
        copy.wait()
    half_rows = rows // 2

    @pl.loop(0, n)
    def _(step):
        @pl.when(step == 1)
        def _():
            forward(0, lside, 0, right)
            forward(1, rside, 2, left)
            forward(0, lside, 4, right)
            forward(0, lside, 1, right)
            forward(1, rside, 3, left)

        @pl.when(step == 2)
        def _():
            for q in (2, 3):
                arrived(0, lside, q)
            for q in (4, 0, 1):
                arrived(1, rside, q)

        @pl.when(step == 3)
        def _():
            for q in (4, 0, 2, 1, 3):
                arrived(2, far, q)

        shift = (3 * step + 3 * (step // 2) + 2 * (step // 3)) % n
        one, two = (me + shift) % n, (me + n - shift) % n
        tokens = jnp.concatenate([a_img[one, :half_rows, :], a_img[two, half_rows:, :]], axis=0)
        project(tokens, w_i, 0, ((pl.multiple_of(one * rows, half_rows), half_rows), (pl.multiple_of(two * rows + half_rows, half_rows), half_rows)))

    fill = jnp.zeros((all_rows - img_rows - n * txt_rows, width), txt.dtype)
    project(jnp.concatenate([a_txt[...].reshape(n * txt_rows, width), fill], axis=0), w_t, 1, ((img_rows, all_rows - img_rows),))

    factor = math.log2(math.e) / math.sqrt(head_dim)
    chunks = all_rows // K_BLOCK
    blocks = all_rows // Q_BLOCK

    def query(index, h):
        value = q_s[index // blocks, pl.ds(pl.multiple_of((index % blocks) * Q_BLOCK, Q_BLOCK), Q_BLOCK), :]
        zero = jnp.zeros_like(value)
        return jnp.where(low, value, zero) if h == 0 else jnp.where(low, zero, value)

    def fold(tile):
        return tile.reshape(tile.shape[0] // 8, 8, tile.shape[1])

    def score(index, value, s_ref, ch, top):
        span = slice(ch * K_BLOCK, (ch + 1) * K_BLOCK)
        tile = lax.dot_general(k_s[index // blocks, span, :], value, (((1,), (1,)), ((), ())), preferred_element_type=jnp.float32)
        if ch == chunks - 1:
            tile = tile + jnp.concatenate([key_bias[...]] * (Q_BLOCK // LANES), axis=1)
        s_ref[span, :] = tile
        peak = jnp.max(fold(tile), axis=0)
        return peak if top is None else jnp.maximum(top, peak)

    def weigh(index, h, s_ref, ch, top, norm, out):
        span = slice(ch * K_BLOCK, (ch + 1) * K_BLOCK)
        prob = jnp.exp2((s_ref[span, :] - top) * factor)
        norm = norm + jnp.sum(fold(prob), axis=0)
        out = out + jnp.dot(v_s[index // blocks, h * head_dim:(h + 1) * head_dim, span], prob.astype(jnp.bfloat16), preferred_element_type=jnp.float32)
        return norm, out

    def stage(next_index, next_h, s_next, index, h, s_now, top_now):
        top = None
        value = query(next_index, next_h)
        norm = jnp.zeros((8, Q_BLOCK), jnp.float32)
        out = jnp.zeros((head_dim, Q_BLOCK), jnp.float32)
        for ch in range(chunks):
            top = score(next_index, value, s_next, ch, top)
            norm, out = weigh(index, h, s_now, ch, top_now, norm, out)
        return jnp.max(top, axis=0, keepdims=True), out / jnp.sum(norm, axis=0, keepdims=True)

    def o_copies(p, d, owner):
        member = (me + d) % n
        lanes = pl.ds(pl.multiple_of(owner * cols + p * LANES, LANES), LANES)
        sources = (o_s.at[p, pl.ds(pl.multiple_of(member * rows, rows), rows)], o_s.at[p, pl.ds(pl.multiple_of(img_rows + member * txt_rows, 16), txt_rows)])
        return list(zip(sources, (img_o.at[:, lanes], txt_o.at[:, lanes])))

    def o_remote(p, d, owner):
        return [remote(src, dst, o_send.at[p, d, t], o_recv.at[p, d, t], *peer(d)) for t, (src, dst) in enumerate(o_copies(p, d, owner))]

    top = None
    value = query(0, 0)
    for ch in range(chunks):
        top = score(0, value, s_a, ch, top)
    top = jnp.max(top, axis=0, keepdims=True)
    steps = pairs * blocks

    def body(step, top_a):
        after = (step + 1) % steps
        top_b, out_a = stage(step, 1, s_b, step, 0, s_a, top_a)
        top_a, out_b = stage(after, 0, s_a, step, 1, s_b, top_b)
        p, b = step // blocks, step % blocks
        o_s[p, pl.ds(pl.multiple_of(b * Q_BLOCK, Q_BLOCK), Q_BLOCK), :] = jnp.concatenate([out_a, out_b], axis=0).T.astype(jnp.bfloat16)

        @pl.when(b == blocks - 1)
        def _():
            for d in (2, 1, 3):
                for copy in o_remote(p, d, me):
                    copy.start()
            for t, (src, dst) in enumerate(o_copies(p, 0, me)):
                pltpu.make_async_copy(src, dst, o_send.at[p, 0, t]).start()

        return top_a

    lax.fori_loop(0, steps, body, top)
    for copy in copies:
        copy.wait_send()
    for kind, slot, q, target in ((0, lside, 0, right), (1, rside, 2, left), (0, lside, 1, right), (1, rside, 3, left), (0, lside, 4, right)):
        remote(landing(slot, q), landing(slot, q), send.at[2, q], recv.at[2, q], *target).wait_send()
    for p in range(pairs):
        for t, (src, dst) in enumerate(o_copies(p, 0, me)):
            pltpu.make_async_copy(src, dst, o_send.at[p, 0, t]).wait()
        for d in range(1, n):
            for copy in o_remote(p, d, me):
                copy.wait_send()
            for copy in o_remote(p, d, (me + n - d) % n):
                copy.wait_recv()


def joint(mesh, img, txt, w_qkv, bias, gain, key_bias, block, head_dim, collective_id):
    n = mesh.shape['u']
    width = img.shape[1]
    all_rows = n * img.shape[0] + TXT_ROWS
    cols = width // n
    pairs = cols // LANES
    bf16, f32 = jnp.bfloat16, jnp.float32
    vmem = pl.BlockSpec(memory_space=VMEM)
    return pl.pallas_call(
        functools.partial(joint_kernel, n, head_dim, block),
        out_shape=[jax.ShapeDtypeStruct(img.shape, bf16), jax.ShapeDtypeStruct(txt.shape, bf16)],
        in_specs=[vmem, vmem, pl.BlockSpec(memory_space=pl.ANY), vmem, vmem, vmem],
        out_specs=[vmem, vmem],
        scratch_shapes=[
            pltpu.VMEM((n,) + img.shape, bf16), pltpu.VMEM((n,) + txt.shape, bf16),
            pltpu.VMEM((width, 3 * cols), bf16), pltpu.VMEM((width, 3 * cols), bf16),
            pltpu.VMEM((pairs, all_rows, LANES), bf16), pltpu.VMEM((pairs, all_rows, LANES), bf16), pltpu.VMEM((pairs, LANES, all_rows), bf16),
            pltpu.VMEM((all_rows, Q_BLOCK), f32), pltpu.VMEM((all_rows, Q_BLOCK), f32),
            pltpu.VMEM((pairs, all_rows, LANES), bf16),
            pltpu.SemaphoreType.DMA((3, 5)), pltpu.SemaphoreType.DMA((3, 5)),
            pltpu.SemaphoreType.DMA((pairs, n, 2)), pltpu.SemaphoreType.DMA((pairs, n, 2)),
            pltpu.SemaphoreType.DMA((8,)),
        ],
        compiler_params=pltpu.CompilerParams(collective_id=collective_id, has_side_effects=True, vmem_limit_bytes=60 * 2**20),
        cost_estimate=pl.CostEstimate(flops=4 * 10**10, bytes_accessed=10**7, transcendentals=0),
        name='joint',
    )(img, txt, w_qkv, bias, gain, key_bias)


def modulated_norm(hidden, shift, scale):
    wide = hidden.astype(jnp.float32)
    centered = wide - jnp.mean(wide, axis=-1, keepdims=True)
    variance = jnp.mean(centered * centered, axis=-1, keepdims=True)
    return ((1.0 + scale) * (centered * lax.rsqrt(variance + EPSILON)) + shift).astype(jnp.bfloat16)


def linear(rows, weight, bias):
    return jnp.dot(rows, weight, preferred_element_type=jnp.float32) + bias.astype(jnp.float32)


def modality_out(hidden, attended, mod, w_proj, b_proj, w_up, b_up, w_down, b_down):
    residual = hidden.astype(jnp.float32) + mod[2] * linear(attended, w_proj, b_proj)
    hidden = residual.astype(jnp.bfloat16)
    normed = modulated_norm(hidden, mod[3], mod[4])
    inner = jax.nn.gelu(linear(normed, w_up, b_up), approximate=True).astype(jnp.bfloat16)
    return (hidden.astype(jnp.float32) + mod[5] * linear(inner, w_down, b_down)).astype(jnp.bfloat16)


def solution(mesh):
    seq_spec = P('dp', ('r', 'u'), None)
    row_spec = P('dp', None)
    n = mesh.shape['u']
    total = n * mesh.shape['r']

    def local_blocks(image, text, cond_vec, key_valid, w_mod, b_mod, w_qkv, b_qkv, q_gain, k_gain, w_proj, b_proj, w_up, b_up, w_down, b_down):
        blocks, _, width, mod_width = w_mod.shape
        heads, head_dim = q_gain.shape[2:]
        r, u = lax.axis_index('r'), lax.axis_index('u')
        c, x = r % 2, r // 2
        sample = jnp.where(c == 0, u, n + x)
        member = jnp.where(c == 0, x, u)
        silu_vec = jax.nn.silu(cond_vec.astype(jnp.float32)).astype(jnp.bfloat16)
        per = blocks * 2 * mod_width // total
        parts = mod_width // per
        me = r * n + u
        which, col = me // parts, (me % parts) * per
        w_mine = lax.dynamic_slice(w_mod, (which // 2, which % 2, 0, col), (1, 1, width, per))[0, 0]
        b_mine = lax.dynamic_slice(b_mod, (which // 2, which % 2, col), (1, 1, per))[0, 0]
        mod_mine = jnp.dot(silu_vec, w_mine, preferred_element_type=jnp.float32) + b_mine.astype(jnp.float32)
        img, txt, mod_all = scatter(mesh, image, text, mod_mine.reshape(-1, per // LANES, LANES))
        mod_all = mod_all.reshape(blocks, 2, 6, 1, width)
        slots, run, _ = img.shape
        txt_run = txt.shape[1]
        img = img.reshape(slots * run, width)
        txt = jnp.pad(txt.reshape(slots * txt_run, width), ((0, TXT_PAD - slots * txt_run), (0, 0)))

        valid = lax.dynamic_slice(key_valid, (sample, 0), (1, key_valid.shape[1]))[0]
        strided = valid.reshape(2 * n, n, txt_run).transpose(1, 0, 2).reshape(-1)
        valid = jnp.where(c == 0, valid, strided).reshape(n, slots * txt_run)
        text_bias = jnp.pad(jnp.where(valid > 0, 0.0, MASK_FILL), ((0, 0), (0, TXT_PAD - slots * txt_run)), constant_values=MASK_FILL).reshape(1, -1)
        text_bias = jnp.pad(text_bias, ((0, 0), (0, TXT_ROWS - n * TXT_PAD)), constant_values=MASK_FILL).astype(jnp.float32)
        key_bias = jnp.broadcast_to(text_bias.reshape(-1, 1), (TXT_ROWS, LANES))

        bias_all = b_qkv.astype(jnp.float32).reshape(blocks, 2, 3, n, width // n)
        bias_all = lax.dynamic_index_in_dim(bias_all, member, 3, keepdims=False).reshape(blocks, 2, -1)
        gain_all = jnp.stack([q_gain, k_gain], axis=2).astype(jnp.float32).reshape(blocks, 2, 2, n, width // n)
        gain_all = lax.dynamic_index_in_dim(gain_all, member, 3, keepdims=False).reshape(blocks, 2, -1)

        sides = [img, txt]
        for block in range(blocks):
            normed = [modulated_norm(sides[s], mod_all[block, s, 0], mod_all[block, s, 1]) for s in range(2)]
            attended = joint(mesh, normed[0], normed[1], w_qkv, bias_all[block], gain_all[block], key_bias, block, head_dim, 2 + block)
            sides = [modality_out(sides[s], attended[s], mod_all[block, s], w_proj[block, s], b_proj[block, s], w_up[block, s], b_up[block, s], w_down[block, s], b_down[block, s]) for s in range(2)]
        img = sides[0].reshape(slots, run, width)
        txt = sides[1][: slots * txt_run].reshape(slots, txt_run, width)
        return unscatter(mesh, img, txt)

    return jax.shard_map(local_blocks, mesh=mesh, in_specs=(seq_spec, seq_spec, row_spec, row_spec) + (P(),) * 12, out_specs=(seq_spec, seq_spec), check_vma=False)
```

```python
import functools
import math

import jax
import jax.numpy as jnp
from jax import lax
from jax.experimental import pallas as pl
from jax.experimental.pallas import tpu as pltpu
from jax.sharding import PartitionSpec as P

EPSILON = 1e-6
MASK_FILL = -1e30
MESH = pl.DeviceIdType.MESH
VMEM = pltpu.VMEM
LANES = 128
TXT_PAD = 48
TXT_ROWS = 256
Q_BLOCK = 768
K_BLOCK = 256
MLP_TILE = 1024
ROW_BLOCK = 512
NORM_ROWS = 128


def place():
    r, u = lax.axis_index('r'), lax.axis_index('u')
    return r, u, r % 2, r // 2


def pick(c, even, odd):
    return (1 - c) * even + c * odd


def remote(src, dst, send, recv, r, u):
    return pltpu.make_async_remote_copy(src_ref=src, dst_ref=dst, send_sem=send, recv_sem=recv, device_id={'r': r, 'u': u}, device_id_type=MESH)


def hello(peers):
    for r, u in peers:
        pl.semaphore_signal(pltpu.get_barrier_semaphore(), inc=1, device_id={'r': r, 'u': u}, device_id_type=MESH)


def greet(peers, count):
    hello(peers)
    pl.semaphore_wait(pltpu.get_barrier_semaphore(), count)


def modulated_norm(hidden, shift, scale):
    wide = hidden.astype(jnp.float32)
    centered = wide - jnp.mean(wide, axis=-1, keepdims=True)
    variance = jnp.mean(centered * centered, axis=-1, keepdims=True)
    return ((1.0 + scale) * (centered * lax.rsqrt(variance + EPSILON)) + shift).astype(jnp.bfloat16)


def scatter_kernel(n, img, txt, mod, img_o, txt_o, mod_o, send, recv, mod_send, mod_recv, local):
    r, u, c, x = place()
    total = 2 * n * n
    me = r * n + u
    others = [(me + d) % total for d in range(1, total)]
    greet([(o // n, o % n) for o in others], total - 1)
    copies = []
    for d, o in enumerate(others):
        ro, uo = o // n, o % n
        sample = pick(ro % 2, uo, n + ro // 2)
        copies.append(remote(mod.at[sample], mod_o.at[me], mod_send.at[d], mod_recv.at[d], ro, uo))
    own_slot = pick(c, u, r)
    targets = []
    for d in list(range(1, n)):
        targets.append((pick(c, r, 2 * ((x + d) % n) + 1), pick(c, (u + d) % n, u), pick(c, (u + d) % n, n + (x + d) % n), own_slot))
    for d in range(n):
        j = (pick(c, x, u) + d) % n
        targets.append((pick(c, 2 * j + 1, 2 * x), pick(c, u, j), pick(c, n + j, j), pick(c, r, n + u)))
    for t, (ro, uo, sample, slot) in enumerate(targets):
        copies.append(remote(img.at[sample], img_o.at[slot], send.at[0, t], recv.at[0, slot], ro, uo))
        copies.append(remote(txt.at[sample], txt_o.at[slot], send.at[1, t], recv.at[1, slot], ro, uo))
    for copy in copies:
        copy.start()
    own_sample = pick(c, u, n + x)
    mine = [
        pltpu.make_async_copy(img.at[own_sample], img_o.at[own_slot], local.at[0]),
        pltpu.make_async_copy(txt.at[own_sample], txt_o.at[own_slot], local.at[1]),
        pltpu.make_async_copy(mod.at[own_sample], mod_o.at[me], local.at[2]),
    ]
    for copy in mine:
        copy.start()
    for copy in copies:
        copy.wait_send()
    for copy in mine:
        copy.wait()
    for d in range(1, total):
        source = (me - d + total) % total
        remote(mod.at[0], mod_o.at[source], mod_send.at[d - 1], mod_recv.at[d - 1], r, u).wait_recv()
    for d in range(1, 2 * n):
        slot = (own_slot + d) % (2 * n)
        remote(img.at[0], img_o.at[slot], send.at[0, 0], recv.at[0, slot], r, u).wait_recv()
        remote(txt.at[0], txt_o.at[slot], send.at[1, 0], recv.at[1, slot], r, u).wait_recv()


def scatter(mesh, img, txt, mod):
    n = mesh.shape['u']
    total = 2 * n * n
    return pl.pallas_call(
        functools.partial(scatter_kernel, n),
        out_shape=[jax.ShapeDtypeStruct(img.shape, img.dtype), jax.ShapeDtypeStruct(txt.shape, txt.dtype), jax.ShapeDtypeStruct((total,) + mod.shape[1:], mod.dtype)],
        in_specs=[pl.BlockSpec(memory_space=VMEM)] * 3,
        out_specs=[pl.BlockSpec(memory_space=VMEM)] * 3,
        scratch_shapes=[pltpu.SemaphoreType.DMA((2, 2 * n)), pltpu.SemaphoreType.DMA((2, 2 * n)), pltpu.SemaphoreType.DMA((total,)), pltpu.SemaphoreType.DMA((total,)), pltpu.SemaphoreType.DMA((3,))],
        compiler_params=pltpu.CompilerParams(collective_id=0, has_side_effects=True),
        name='scatter',
    )(img, txt, mod)


def unscatter_kernel(n, img, txt, img_o, txt_o, send, recv, local):
    r, u, c, x = place()
    own_slot, sample = pick(c, u, r), pick(c, u, n + x)
    senders, targets = [], []
    for d in range(1, 2 * n):
        s = (sample + d) % (2 * n)
        odd = s // n
        senders.append((pick(odd, 2 * x, 2 * (s % n) + 1), pick(odd, s, u)))
        k = (own_slot + d) % (2 * n)
        targets.append((pick(c, 2 * x + k // n, k), pick(c, k % n, u), k))
    greet(senders, 2 * n - 1)
    copies = []
    for t, (ro, uo, k) in enumerate(targets):
        copies.append(remote(img.at[k], img_o.at[sample], send.at[0, t], recv.at[0, sample], ro, uo))
        copies.append(remote(txt.at[k], txt_o.at[sample], send.at[1, t], recv.at[1, sample], ro, uo))
    for copy in copies:
        copy.start()
    mine = [pltpu.make_async_copy(img.at[own_slot], img_o.at[sample], local.at[0]), pltpu.make_async_copy(txt.at[own_slot], txt_o.at[sample], local.at[1])]
    for copy in mine:
        copy.start()
    for copy in copies:
        copy.wait_send()
    for copy in mine:
        copy.wait()
    for d in range(1, 2 * n):
        s = (sample + d) % (2 * n)
        remote(img.at[0], img_o.at[s], send.at[0, 0], recv.at[0, s], r, u).wait_recv()
        remote(txt.at[0], txt_o.at[s], send.at[1, 0], recv.at[1, s], r, u).wait_recv()


def unscatter(mesh, img, txt):
    n = mesh.shape['u']
    return pl.pallas_call(
        functools.partial(unscatter_kernel, n),
        out_shape=[jax.ShapeDtypeStruct(img.shape, img.dtype), jax.ShapeDtypeStruct(txt.shape, txt.dtype)],
        in_specs=[pl.BlockSpec(memory_space=VMEM)] * 2,
        out_specs=[pl.BlockSpec(memory_space=VMEM)] * 2,
        scratch_shapes=[pltpu.SemaphoreType.DMA((2, 2 * n)), pltpu.SemaphoreType.DMA((2, 2 * n)), pltpu.SemaphoreType.DMA((2,))],
        compiler_params=pltpu.CompilerParams(collective_id=1, has_side_effects=True),
        name='unscatter',
    )(img, txt)


def ring_place(n):
    r, u, c, x = place()
    me = pick(c, x, u)

    def peer(d):
        j = (me + d + n) % n
        return pick(c, 2 * j, r), pick(c, u, j)

    return me, peer


def joint_kernel(n, head_dim, block, x_img, x_txt, mod, w_qkv, bias, gain, key_bias, img_o, txt_o, a_img, a_txt, w_i, w_t, q_s, k_s, v_s, s_a, s_b, o_s, send, recv, o_send, o_recv, local):
    me, peer = ring_place(n)
    right, left = peer(1), peer(-1)
    rows, width = x_img.shape
    txt_rows = x_txt.shape[0]
    img_rows = n * rows
    img, txt = a_img.at[me], a_txt.at[me]
    pairs, all_rows = q_s.shape[:2]
    cols = pairs * LANES
    weights = []
    for side, ref in ((0, w_i), (1, w_t)):
        for t in range(3):
            start = pl.multiple_of(t * width + me * cols, LANES)
            weights.append(pltpu.make_async_copy(w_qkv.at[block, side, :, pl.ds(start, cols)], ref.at[:, pl.ds(t * cols, cols)], local.at[2 + 3 * side + t]))
    for copy in weights:
        copy.start()
    hello([peer(d) for d in range(1, n)])
    for side, (source, target) in enumerate(((x_txt, a_txt), (x_img, a_img))):
        side = 1 - side
        size = min(source.shape[0], NORM_ROWS)

        @pl.loop(0, source.shape[0] // size)
        def _(step):
            span = pl.ds(pl.multiple_of(step * size, size), size)
            target[me, span, :] = modulated_norm(source[span, :], mod[side, 0:1, :], mod[side, 1:2, :])

    pl.semaphore_wait(pltpu.get_barrier_semaphore(), n - 1)
    piece = rows // 4
    lside, rside, far = (me + n - 1) % n, (me + 1) % n, (me + 2) % n

    def part(ref, txt_ref, q):
        return txt_ref if q == 4 else ref.at[pl.ds(q * piece, piece)]

    def landing(slot, q):
        return part(a_img.at[slot], a_txt.at[slot], q)

    copies = []
    for q_right, q_left in zip((0, 1, 4, 2, 3), (2, 3, 4, 0, 1)):
        copies.append(remote(part(img, txt, q_right), landing(me, q_right), send.at[0, q_right], recv.at[0, q_right], *right))
        copies.append(remote(part(img, txt, q_left), landing(me, q_left), send.at[1, q_left], recv.at[1, q_left], *left))
    for copy in copies:
        copy.start()

    def arrived(kind, slot, q):
        remote(landing(slot, q), landing(slot, q), send.at[0, q], recv.at[kind, q], *right).wait_recv()

    def forward(kind, slot, q, target):
        arrived(kind, slot, q)
        copy = remote(landing(slot, q), landing(slot, q), send.at[2, q], recv.at[2, q], *target)
        copy.start()

    low = lax.broadcasted_iota(jnp.int32, (Q_BLOCK, LANES), 1) < head_dim

    def unit(part, scale_by):
        square = part * part
        mask = low[: part.shape[0]]
        first = jnp.sum(jnp.where(mask, square, 0.0), axis=-1, keepdims=True)
        second = jnp.sum(jnp.where(mask, 0.0, square), axis=-1, keepdims=True)
        scale = lax.rsqrt(jnp.where(mask, first, second) * (1.0 / head_dim) + EPSILON)
        return (part * scale * scale_by).astype(jnp.bfloat16)

    def project(tokens, weight, side, spans):
        for tile in range(0, 3 * pairs, 2):
            count = min(2, 3 * pairs - tile)
            lanes = slice(tile * LANES, (tile + count) * LANES)
            packed = jnp.dot(tokens, weight[:, lanes], preferred_element_type=jnp.float32) + bias[side:side + 1, lanes]
            for k in range(count):
                kind, p = (tile + k) // pairs, (tile + k) % pairs
                value = packed[:, k * LANES:(k + 1) * LANES]
                if kind < 2:
                    value = unit(value, gain[side:side + 1, (tile + k) * LANES:(tile + k + 1) * LANES])
                else:
                    value = value.T.astype(jnp.bfloat16)
                offset = 0
                for start, size in spans:
                    if kind == 0:
                        q_s[p, pl.ds(start, size), :] = value[offset:offset + size]
                    elif kind == 1:
                        k_s[p, pl.ds(start, size), :] = value[offset:offset + size]
                    else:
                        v_s[p, :, pl.ds(start, size)] = value[:, offset:offset + size]
                    offset += size

    for copy in weights:
        copy.wait()
    half_rows = rows // 2

    @pl.loop(0, n)
    def _(step):
        @pl.when(step == 1)
        def _():
            forward(0, lside, 0, right)
            forward(1, rside, 2, left)
            forward(0, lside, 4, right)
            forward(0, lside, 1, right)
            forward(1, rside, 3, left)

        @pl.when(step == 2)
        def _():
            for q in (2, 3):
                arrived(0, lside, q)
            for q in (4, 0, 1):
                arrived(1, rside, q)

        @pl.when(step == 3)
        def _():
            for q in (4, 0, 2, 1, 3):
                arrived(2, far, q)

        shift = (3 * step + 3 * (step // 2) + 2 * (step // 3)) % n
        one, two = (me + shift) % n, (me + n - shift) % n
        tokens = jnp.concatenate([a_img[one, :half_rows, :], a_img[two, half_rows:, :]], axis=0)
        project(tokens, w_i, 0, ((pl.multiple_of(one * rows, half_rows), half_rows), (pl.multiple_of(two * rows + half_rows, half_rows), half_rows)))

    fill = jnp.zeros((all_rows - img_rows - n * txt_rows, width), txt.dtype)
    project(jnp.concatenate([a_txt[...].reshape(n * txt_rows, width), fill], axis=0), w_t, 1, ((img_rows, all_rows - img_rows),))

    factor = math.log2(math.e) / math.sqrt(head_dim)
    chunks = all_rows // K_BLOCK
    blocks = all_rows // Q_BLOCK

    def query(index, h):
        value = q_s[index // blocks, pl.ds(pl.multiple_of((index % blocks) * Q_BLOCK, Q_BLOCK), Q_BLOCK), :]
        zero = jnp.zeros_like(value)
        return jnp.where(low, value, zero) if h == 0 else jnp.where(low, zero, value)

    def fold(tile):
        return tile.reshape(tile.shape[0] // 8, 8, tile.shape[1])

    def score(index, value, s_ref, ch, top):
        span = slice(ch * K_BLOCK, (ch + 1) * K_BLOCK)
        tile = lax.dot_general(k_s[index // blocks, span, :], value, (((1,), (1,)), ((), ())), preferred_element_type=jnp.float32)
        if ch == chunks - 1:
            tile = tile + jnp.concatenate([key_bias[...]] * (Q_BLOCK // LANES), axis=1)
        s_ref[span, :] = tile
        peak = jnp.max(fold(tile), axis=0)
        return peak if top is None else jnp.maximum(top, peak)

    def weigh(index, h, s_ref, ch, top, norm, out):
        span = slice(ch * K_BLOCK, (ch + 1) * K_BLOCK)
        prob = jnp.exp2((s_ref[span, :] - top) * factor)
        norm = norm + jnp.sum(fold(prob), axis=0)
        out = out + jnp.dot(v_s[index // blocks, h * head_dim:(h + 1) * head_dim, span], prob.astype(jnp.bfloat16), preferred_element_type=jnp.float32)
        return norm, out

    def stage(next_index, next_h, s_next, index, h, s_now, top_now):
        top = None
        value = query(next_index, next_h)
        norm = jnp.zeros((8, Q_BLOCK), jnp.float32)
        out = jnp.zeros((head_dim, Q_BLOCK), jnp.float32)
        for ch in range(chunks):
            top = score(next_index, value, s_next, ch, top)
            norm, out = weigh(index, h, s_now, ch, top_now, norm, out)
        return jnp.max(top, axis=0, keepdims=True), out / jnp.sum(norm, axis=0, keepdims=True)

    def o_copies(p, d, owner):
        member = (me + d) % n
        lanes = pl.ds(pl.multiple_of(owner * cols + p * LANES, LANES), LANES)
        sources = (o_s.at[p, pl.ds(pl.multiple_of(member * rows, rows), rows)], o_s.at[p, pl.ds(pl.multiple_of(img_rows + member * txt_rows, 16), txt_rows)])
        return list(zip(sources, (img_o.at[:, lanes], txt_o.at[:, lanes])))

    def o_remote(p, d, owner):
        return [remote(src, dst, o_send.at[p, d, t], o_recv.at[p, d, t], *peer(d)) for t, (src, dst) in enumerate(o_copies(p, d, owner))]

    top = None
    value = query(0, 0)
    for ch in range(chunks):
        top = score(0, value, s_a, ch, top)
    top = jnp.max(top, axis=0, keepdims=True)
    steps = pairs * blocks

    def body(step, top_a):
        after = (step + 1) % steps
        top_b, out_a = stage(step, 1, s_b, step, 0, s_a, top_a)
        top_a, out_b = stage(after, 0, s_a, step, 1, s_b, top_b)
        p, b = step // blocks, step % blocks
        o_s[p, pl.ds(pl.multiple_of(b * Q_BLOCK, Q_BLOCK), Q_BLOCK), :] = jnp.concatenate([out_a, out_b], axis=0).T.astype(jnp.bfloat16)

        @pl.when(b == blocks - 1)
        def _():
            for d in (2, 1, 3):
                for copy in o_remote(p, d, me):
                    copy.start()
            for t, (src, dst) in enumerate(o_copies(p, 0, me)):
                pltpu.make_async_copy(src, dst, o_send.at[p, 0, t]).start()

        return top_a

    lax.fori_loop(0, steps, body, top)
    for copy in copies:
        copy.wait_send()
    for kind, slot, q, target in ((0, lside, 0, right), (1, rside, 2, left), (0, lside, 1, right), (1, rside, 3, left), (0, lside, 4, right)):
        remote(landing(slot, q), landing(slot, q), send.at[2, q], recv.at[2, q], *target).wait_send()
    for p in range(pairs):
        for t, (src, dst) in enumerate(o_copies(p, 0, me)):
            pltpu.make_async_copy(src, dst, o_send.at[p, 0, t]).wait()
        for d in range(1, n):
            for copy in o_remote(p, d, me):
                copy.wait_send()
            for copy in o_remote(p, d, (me + n - d) % n):
                copy.wait_recv()


def joint(mesh, img, txt, mod, w_qkv, bias, gain, key_bias, block, head_dim, collective_id):
    n = mesh.shape['u']
    width = img.shape[1]
    all_rows = n * img.shape[0] + TXT_ROWS
    cols = width // n
    pairs = cols // LANES
    bf16, f32 = jnp.bfloat16, jnp.float32
    vmem = pl.BlockSpec(memory_space=VMEM)
    return pl.pallas_call(
        functools.partial(joint_kernel, n, head_dim, block),
        out_shape=[jax.ShapeDtypeStruct(img.shape, bf16), jax.ShapeDtypeStruct(txt.shape, bf16)],
        in_specs=[vmem, vmem, vmem, pl.BlockSpec(memory_space=pl.ANY), vmem, vmem, vmem],
        out_specs=[vmem, vmem],
        scratch_shapes=[
            pltpu.VMEM((n,) + img.shape, bf16), pltpu.VMEM((n,) + txt.shape, bf16),
            pltpu.VMEM((width, 3 * cols), bf16), pltpu.VMEM((width, 3 * cols), bf16),
            pltpu.VMEM((pairs, all_rows, LANES), bf16), pltpu.VMEM((pairs, all_rows, LANES), bf16), pltpu.VMEM((pairs, LANES, all_rows), bf16),
            pltpu.VMEM((all_rows, Q_BLOCK), f32), pltpu.VMEM((all_rows, Q_BLOCK), f32),
            pltpu.VMEM((pairs, all_rows, LANES), bf16),
            pltpu.SemaphoreType.DMA((3, 5)), pltpu.SemaphoreType.DMA((3, 5)),
            pltpu.SemaphoreType.DMA((pairs, n, 2)), pltpu.SemaphoreType.DMA((pairs, n, 2)),
            pltpu.SemaphoreType.DMA((8,)),
        ],
        compiler_params=pltpu.CompilerParams(collective_id=collective_id, has_side_effects=True, vmem_limit_bytes=60 * 2**20),
        cost_estimate=pl.CostEstimate(flops=4 * 10**10, bytes_accessed=10**7, transcendentals=0),
        name='joint',
    )(img, txt, mod, w_qkv, bias, gain, key_bias)


def mlp_kernel(x_i, x_t, o_i, o_t, mod, wp_i, wp_t, wu_i, wu_t, wd_i, wd_t, bias, bias_up_i, bias_up_t, y_i, y_t, r_i, r_t, a_i, a_t, acc_i, acc_t):
    outs = (y_i, y_t)
    step = pl.program_id(0)
    tiles = pl.num_programs(0)
    sides = ((x_i, o_i, wp_i, wu_i, wd_i, bias_up_i, r_i, a_i, acc_i), (x_t, o_t, wp_t, wu_t, wd_t, bias_up_t, r_t, a_t, acc_t))

    def row(ref, side, k):
        return ref[side, k:k + 1, :]

    def row_blocks(ref):
        size = min(ref.shape[0], ROW_BLOCK)
        return [pl.ds(start, size) for start in range(0, ref.shape[0], size)]

    @pl.when(step == 0)
    def _():
        for side, (x, o, wp, wu, wd, bu, r, a, acc) in enumerate(sides):
            for span in row_blocks(x):
                lin = jnp.dot(o[span, :], wp[0, 0], preferred_element_type=jnp.float32) + bias[side, 0:1, :]
                hidden = (x[span, :].astype(jnp.float32) + row(mod, side, 2) * lin).astype(jnp.bfloat16)
                r[span, :] = hidden
                a[span, :] = modulated_norm(hidden, row(mod, side, 3), row(mod, side, 4))
                acc[span, :] = jnp.zeros_like(acc[span, :])

    for side, (x, o, wp, wu, wd, bu, r, a, acc) in enumerate(sides):
        for span in row_blocks(x):
            inner = jnp.dot(a[span, :], wu[0, 0], preferred_element_type=jnp.float32) + bu[0]
            inner = jax.nn.gelu(inner, approximate=True).astype(jnp.bfloat16)
            acc[span, :] += jnp.dot(inner, wd[0, 0], preferred_element_type=jnp.float32)

    @pl.when(step == tiles - 1)
    def _():
        for side, (x, o, wp, wu, wd, bu, r, a, acc) in enumerate(sides):
            for span in row_blocks(x):
                lin = acc[span, :] + bias[side, 1:2, :]
                hidden = (r[span, :].astype(jnp.float32) + row(mod, side, 5) * lin).astype(jnp.bfloat16)
                outs[side][span, :] = hidden


def mlp(sides, attended, mod, w_proj, b_proj, w_up, b_up, w_down, b_down, block):
    width, inner = w_up.shape[2:]
    tiles = inner // MLP_TILE
    bias = jnp.stack([b_proj[block], b_down[block]], axis=1).astype(jnp.float32)
    bias_up = b_up.astype(jnp.float32).reshape(-1, 1, inner)
    whole = lambda shape: pl.BlockSpec(shape, lambda t: (0,) * len(shape))
    sizes = [sides[0].shape, sides[1].shape]
    wp = [pl.BlockSpec((1, 1, width, width), lambda t, s=s: (block, s, 0, 0)) for s in range(2)]
    wu = [pl.BlockSpec((1, 1, width, MLP_TILE), lambda t, s=s: (block, s, 0, t)) for s in range(2)]
    wd = [pl.BlockSpec((1, 1, MLP_TILE, width), lambda t, s=s: (block, s, t, 0)) for s in range(2)]
    bu = [pl.BlockSpec((1, 1, MLP_TILE), lambda t, s=s: (block * 2 + s, 0, t)) for s in range(2)]
    shapes = [jax.ShapeDtypeStruct(size, jnp.bfloat16) for size in sizes]
    scratch = [pltpu.VMEM(size, dtype) for dtype in (jnp.bfloat16, jnp.bfloat16, jnp.float32) for size in sizes]
    return pl.pallas_call(
        mlp_kernel,
        out_shape=shapes,
        grid=(tiles,),
        in_specs=[whole(s) for s in sizes] * 2 + [whole(mod.shape)] + wp + wu + wd + [whole(bias.shape)] + bu,
        out_specs=[whole(s.shape) for s in shapes],
        scratch_shapes=scratch,
        compiler_params=pltpu.CompilerParams(vmem_limit_bytes=60 * 2**20, dimension_semantics=('arbitrary',)),
        cost_estimate=pl.CostEstimate(flops=25 * 10**9, bytes_accessed=86 * 10**6, transcendentals=0),
        name='mlp',
    )(sides[0], sides[1], attended[0], attended[1], mod, w_proj, w_proj, w_up, w_up, w_down, w_down, bias, bias_up, bias_up)


def solution(mesh):
    seq_spec = P('dp', ('r', 'u'), None)
    row_spec = P('dp', None)
    n = mesh.shape['u']
    total = n * mesh.shape['r']

    def local_blocks(image, text, cond_vec, key_valid, w_mod, b_mod, w_qkv, b_qkv, q_gain, k_gain, w_proj, b_proj, w_up, b_up, w_down, b_down):
        blocks, _, width, mod_width = w_mod.shape
        heads, head_dim = q_gain.shape[2:]
        r, u = lax.axis_index('r'), lax.axis_index('u')
        c, x = r % 2, r // 2
        sample = jnp.where(c == 0, u, n + x)
        member = jnp.where(c == 0, x, u)
        silu_vec = jax.nn.silu(cond_vec.astype(jnp.float32)).astype(jnp.bfloat16)
        per = blocks * 2 * mod_width // total
        parts = mod_width // per
        me = r * n + u
        which, col = me // parts, (me % parts) * per
        w_mine = lax.dynamic_slice(w_mod, (which // 2, which % 2, 0, col), (1, 1, width, per))[0, 0]
        b_mine = lax.dynamic_slice(b_mod, (which // 2, which % 2, col), (1, 1, per))[0, 0]
        mod_mine = jnp.dot(silu_vec, w_mine, preferred_element_type=jnp.float32) + b_mine.astype(jnp.float32)
        img, txt, mod_all = scatter(mesh, image, text, mod_mine.reshape(-1, per // LANES, LANES))
        mod_all = mod_all.reshape(blocks, 2, 6, width)
        slots, run, _ = img.shape
        txt_run = txt.shape[1]
        img = img.reshape(slots * run, width)
        txt = jnp.pad(txt.reshape(slots * txt_run, width), ((0, TXT_PAD - slots * txt_run), (0, 0)))

        valid = lax.dynamic_slice(key_valid, (sample, 0), (1, key_valid.shape[1]))[0]
        strided = valid.reshape(2 * n, n, txt_run).transpose(1, 0, 2).reshape(-1)
        valid = jnp.where(c == 0, valid, strided).reshape(n, slots * txt_run)
        text_bias = jnp.pad(jnp.where(valid > 0, 0.0, MASK_FILL), ((0, 0), (0, TXT_PAD - slots * txt_run)), constant_values=MASK_FILL).reshape(1, -1)
        text_bias = jnp.pad(text_bias, ((0, 0), (0, TXT_ROWS - n * TXT_PAD)), constant_values=MASK_FILL).astype(jnp.float32)
        key_bias = jnp.broadcast_to(text_bias.reshape(-1, 1), (TXT_ROWS, LANES))

        bias_all = b_qkv.astype(jnp.float32).reshape(blocks, 2, 3, n, width // n)
        bias_all = lax.dynamic_index_in_dim(bias_all, member, 3, keepdims=False).reshape(blocks, 2, -1)
        gain_all = jnp.stack([q_gain, k_gain], axis=2).astype(jnp.float32).reshape(blocks, 2, 2, n, width // n)
        gain_all = lax.dynamic_index_in_dim(gain_all, member, 3, keepdims=False).reshape(blocks, 2, -1)

        sides = [img, txt]
        for block in range(blocks):
            attended = joint(mesh, sides[0], sides[1], mod_all[block], w_qkv, bias_all[block], gain_all[block], key_bias, block, head_dim, 2 + block)
            sides = mlp(sides, attended, mod_all[block], w_proj, b_proj, w_up, b_up, w_down, b_down, block)
        img = sides[0].reshape(slots, run, width)
        txt = sides[1][: slots * txt_run].reshape(slots, txt_run, width)
        return unscatter(mesh, img, txt)

    return jax.shard_map(local_blocks, mesh=mesh, in_specs=(seq_spec, seq_spec, row_spec, row_spec) + (P(),) * 12, out_specs=(seq_spec, seq_spec), check_vma=False)
```

```python
import functools
import math

import jax
import jax.numpy as jnp
from jax import lax
from jax.experimental import pallas as pl
from jax.experimental.pallas import tpu as pltpu
from jax.sharding import PartitionSpec as P

EPSILON = 1e-6
MASK_FILL = -1e30
MESH = pl.DeviceIdType.MESH
VMEM = pltpu.VMEM
LANES = 128
TXT_PAD = 48
TXT_ROWS = 256
Q_BLOCK = 768
K_BLOCK = 256
MLP_TILE = 1024
ROW_BLOCK = 512
NORM_ROWS = 128


def place():
    r, u = lax.axis_index('r'), lax.axis_index('u')
    return r, u, r % 2, r // 2


def pick(c, even, odd):
    return (1 - c) * even + c * odd


def remote(src, dst, send, recv, r, u):
    return pltpu.make_async_remote_copy(src_ref=src, dst_ref=dst, send_sem=send, recv_sem=recv, device_id={'r': r, 'u': u}, device_id_type=MESH)


def hello(peers):
    for r, u in peers:
        pl.semaphore_signal(pltpu.get_barrier_semaphore(), inc=1, device_id={'r': r, 'u': u}, device_id_type=MESH)


def greet(peers, count):
    hello(peers)
    pl.semaphore_wait(pltpu.get_barrier_semaphore(), count)


def modulated_norm(hidden, shift, scale):
    wide = hidden.astype(jnp.float32)
    centered = wide - jnp.mean(wide, axis=-1, keepdims=True)
    variance = jnp.mean(centered * centered, axis=-1, keepdims=True)
    return ((1.0 + scale) * (centered * lax.rsqrt(variance + EPSILON)) + shift).astype(jnp.bfloat16)


def scatter_kernel(n, img, txt, cond, w_mod, b_mod, img_o, txt_o, mod_o, w_s, mod, send, recv, mod_send, mod_recv, local):
    r, u, c, x = place()
    total = 2 * n * n
    me = r * n + u
    per = w_s.shape[1]
    parts = w_mod.shape[3] // per
    which = me // parts
    block, side = which // w_mod.shape[1], which % w_mod.shape[1]
    span = pl.ds(pl.multiple_of((me % parts) * per, LANES), per)
    weight = pltpu.make_async_copy(w_mod.at[block, side, :, span], w_s, local.at[2])
    weight.start()
    others = [(me + d) % total for d in range(1, total)]
    greet([(o // n, o % n) for o in others], total - 1)
    copies = []
    own_slot = pick(c, u, r)
    targets = []
    for d in (2, 1, 3):
        targets.append((pick(c, r, 2 * ((x + d) % n) + 1), pick(c, (u + d) % n, u), pick(c, (u + d) % n, n + (x + d) % n), own_slot))
    for d in (2, 1, 3, 0):
        j = (pick(c, x, u) + d) % n
        targets.append((pick(c, 2 * j + 1, 2 * x), pick(c, u, j), pick(c, n + j, j), pick(c, r, n + u)))
    for t, (ro, uo, sample, slot) in enumerate(targets):
        copies.append(remote(img.at[sample], img_o.at[slot], send.at[0, t], recv.at[0, slot], ro, uo))
        copies.append(remote(txt.at[sample], txt_o.at[slot], send.at[1, t], recv.at[1, slot], ro, uo))
    for copy in copies:
        copy.start()
    own_sample = pick(c, u, n + x)
    mine = [
        pltpu.make_async_copy(img.at[own_sample], img_o.at[own_slot], local.at[0]),
        pltpu.make_async_copy(txt.at[own_sample], txt_o.at[own_slot], local.at[1]),
    ]
    for copy in mine:
        copy.start()
    silu_vec = jax.nn.silu(cond[...].astype(jnp.float32)).astype(jnp.bfloat16)
    both = b_mod[block, :, span].astype(jnp.float32)
    picked = lax.broadcasted_iota(jnp.int32, both.shape, 0) == side
    bias = jnp.sum(jnp.where(picked, both, 0.0), axis=0, keepdims=True)
    weight.wait()
    vecs = jnp.dot(silu_vec, w_s[...], preferred_element_type=jnp.float32) + bias
    for k in range(per // LANES):
        mod[:, k, :] = vecs[:, k * LANES:(k + 1) * LANES]
    rows = []
    for d, o in enumerate(others):
        ro, uo = o // n, o % n
        sample = pick(ro % 2, uo, n + ro // 2)
        rows.append(remote(mod.at[sample], mod_o.at[me], mod_send.at[d], mod_recv.at[d], ro, uo))
    for copy in rows:
        copy.start()
    mod_o[me] = mod[own_sample]
    for copy in copies + rows:
        copy.wait_send()
    for copy in mine:
        copy.wait()
    for d in range(1, total):
        source = (me - d + total) % total
        remote(mod.at[0], mod_o.at[source], mod_send.at[d - 1], mod_recv.at[d - 1], r, u).wait_recv()
    for d in range(1, 2 * n):
        slot = (own_slot + d) % (2 * n)
        remote(img.at[0], img_o.at[slot], send.at[0, 0], recv.at[0, slot], r, u).wait_recv()
        remote(txt.at[0], txt_o.at[slot], send.at[1, 0], recv.at[1, slot], r, u).wait_recv()


def scatter(mesh, img, txt, cond, w_mod, b_mod):
    n = mesh.shape['u']
    total = 2 * n * n
    width = cond.shape[1]
    per = w_mod.shape[0] * w_mod.shape[1] * w_mod.shape[3] // total
    rows = (per // LANES, LANES)
    return pl.pallas_call(
        functools.partial(scatter_kernel, n),
        out_shape=[jax.ShapeDtypeStruct(img.shape, img.dtype), jax.ShapeDtypeStruct(txt.shape, txt.dtype), jax.ShapeDtypeStruct((total,) + rows, jnp.float32)],
        in_specs=[pl.BlockSpec(memory_space=VMEM)] * 3 + [pl.BlockSpec(memory_space=pl.ANY), pl.BlockSpec(memory_space=VMEM)],
        out_specs=[pl.BlockSpec(memory_space=VMEM)] * 3,
        scratch_shapes=[pltpu.VMEM((width, per), w_mod.dtype), pltpu.VMEM((cond.shape[0],) + rows, jnp.float32), pltpu.SemaphoreType.DMA((2, 2 * n)), pltpu.SemaphoreType.DMA((2, 2 * n)), pltpu.SemaphoreType.DMA((total,)), pltpu.SemaphoreType.DMA((total,)), pltpu.SemaphoreType.DMA((3,))],
        compiler_params=pltpu.CompilerParams(collective_id=0, has_side_effects=True),
        name='scatter',
    )(img, txt, cond, w_mod, b_mod)


def unscatter_kernel(n, img, txt, img_o, txt_o, send, recv, local):
    r, u, c, x = place()
    own_slot, sample = pick(c, u, r), pick(c, u, n + x)
    senders, targets = [], []
    for d in range(1, 2 * n):
        s = (sample + d) % (2 * n)
        odd = s // n
        senders.append((pick(odd, 2 * x, 2 * (s % n) + 1), pick(odd, s, u)))
        k = (own_slot + d) % (2 * n)
        targets.append((pick(c, 2 * x + k // n, k), pick(c, k % n, u), k))
    greet(senders, 2 * n - 1)
    copies = []
    for t, (ro, uo, k) in enumerate(targets):
        copies.append(remote(img.at[k], img_o.at[sample], send.at[0, t], recv.at[0, sample], ro, uo))
        copies.append(remote(txt.at[k], txt_o.at[sample], send.at[1, t], recv.at[1, sample], ro, uo))
    for copy in copies:
        copy.start()
    mine = [pltpu.make_async_copy(img.at[own_slot], img_o.at[sample], local.at[0]), pltpu.make_async_copy(txt.at[own_slot], txt_o.at[sample], local.at[1])]
    for copy in mine:
        copy.start()
    for copy in copies:
        copy.wait_send()
    for copy in mine:
        copy.wait()
    for d in range(1, 2 * n):
        s = (sample + d) % (2 * n)
        remote(img.at[0], img_o.at[s], send.at[0, 0], recv.at[0, s], r, u).wait_recv()
        remote(txt.at[0], txt_o.at[s], send.at[1, 0], recv.at[1, s], r, u).wait_recv()


def unscatter(mesh, img, txt):
    n = mesh.shape['u']
    return pl.pallas_call(
        functools.partial(unscatter_kernel, n),
        out_shape=[jax.ShapeDtypeStruct(img.shape, img.dtype), jax.ShapeDtypeStruct(txt.shape, txt.dtype)],
        in_specs=[pl.BlockSpec(memory_space=VMEM)] * 2,
        out_specs=[pl.BlockSpec(memory_space=VMEM)] * 2,
        scratch_shapes=[pltpu.SemaphoreType.DMA((2, 2 * n)), pltpu.SemaphoreType.DMA((2, 2 * n)), pltpu.SemaphoreType.DMA((2,))],
        compiler_params=pltpu.CompilerParams(collective_id=1, has_side_effects=True),
        name='unscatter',
    )(img, txt)


def ring_place(n):
    r, u, c, x = place()
    me = pick(c, x, u)

    def peer(d):
        j = (me + d + n) % n
        return pick(c, 2 * j, r), pick(c, u, j)

    return me, peer


def joint_kernel(n, head_dim, txt_run, block, x_img, x_txt, mod, w_qkv, b_qkv, q_gain, k_gain, valid, img_o, txt_o, bias, gain, key_bias, a_img, a_txt, w_i, w_t, q_s, k_s, v_s, s_a, s_b, o_s, send, recv, o_send, o_recv, local):
    me, peer = ring_place(n)
    right, left = peer(1), peer(-1)
    rows, width = x_img.shape
    txt_rows = x_txt.shape[0]
    img_rows = n * rows
    img, txt = a_img.at[me], a_txt.at[me]
    pairs, all_rows = q_s.shape[:2]
    cols = pairs * LANES
    weights = []
    for side, ref in ((0, w_i), (1, w_t)):
        for t in range(3):
            start = pl.multiple_of(t * width + me * cols, LANES)
            weights.append(pltpu.make_async_copy(w_qkv.at[block, side, :, pl.ds(start, cols)], ref.at[:, pl.ds(t * cols, cols)], local.at[2 + 3 * side + t]))
    for copy in weights:
        copy.start()
    hello([peer(d) for d in range(1, n)])
    for side, (source, target) in enumerate(((x_txt, a_txt), (x_img, a_img))):
        side = 1 - side
        size = min(source.shape[0], NORM_ROWS)

        @pl.loop(0, source.shape[0] // size)
        def _(step):
            span = pl.ds(pl.multiple_of(step * size, size), size)
            target[me, span, :] = modulated_norm(source[span, :], mod[side, 0:1, :], mod[side, 1:2, :])

    pl.semaphore_wait(pltpu.get_barrier_semaphore(), n - 1)
    piece = rows // 4
    lside, rside, far = (me + n - 1) % n, (me + 1) % n, (me + 2) % n

    def part(ref, txt_ref, q):
        return txt_ref if q == 4 else ref.at[pl.ds(q * piece, piece)]

    def landing(slot, q):
        return part(a_img.at[slot], a_txt.at[slot], q)

    copies = []
    for q_right, q_left in zip((0, 1, 4, 2, 3), (2, 3, 4, 0, 1)):
        copies.append(remote(part(img, txt, q_right), landing(me, q_right), send.at[0, q_right], recv.at[0, q_right], *right))
        copies.append(remote(part(img, txt, q_left), landing(me, q_left), send.at[1, q_left], recv.at[1, q_left], *left))
    for copy in copies:
        copy.start()

    def arrived(kind, slot, q):
        remote(landing(slot, q), landing(slot, q), send.at[0, q], recv.at[kind, q], *right).wait_recv()

    def forward(kind, slot, q, target):
        arrived(kind, slot, q)
        copy = remote(landing(slot, q), landing(slot, q), send.at[2, q], recv.at[2, q], *target)
        copy.start()

    own = pl.ds(pl.multiple_of(me * cols, LANES), cols)
    for t in range(3):
        third = pl.ds(pl.multiple_of(t * width + me * cols, LANES), cols)
        bias[:, t * cols:(t + 1) * cols] = b_qkv[block, :, third].astype(jnp.float32)
    for t, ref in enumerate((q_gain, k_gain)):
        gain[:, t * cols:(t + 1) * cols] = ref[block, :, own].astype(jnp.float32)
    r, u, c, x = place()
    count = jnp.sum(valid[pl.ds(pick(c, u, n + x), 1), :], axis=-1, keepdims=True)
    index = lax.broadcasted_iota(jnp.int32, key_bias.shape, 0)
    member, inside = index // txt_rows, index % txt_rows
    token = (1 - c) * (member * (2 * n * txt_run) + inside) + c * ((inside // txt_run * n + member) * txt_run + inside % txt_run)
    seen = (inside < 2 * n * txt_run) & (member < n) & (token.astype(jnp.float32) < count)
    key_bias[...] = jnp.where(seen, 0.0, MASK_FILL)

    low = lax.broadcasted_iota(jnp.int32, (Q_BLOCK, LANES), 1) < head_dim

    def unit(part, scale_by):
        square = part * part
        mask = low[: part.shape[0]]
        first = jnp.sum(jnp.where(mask, square, 0.0), axis=-1, keepdims=True)
        second = jnp.sum(jnp.where(mask, 0.0, square), axis=-1, keepdims=True)
        scale = lax.rsqrt(jnp.where(mask, first, second) * (1.0 / head_dim) + EPSILON)
        return (part * scale * scale_by).astype(jnp.bfloat16)

    def project(tokens, weight, side, spans):
        for tile in range(0, 3 * pairs, 2):
            count = min(2, 3 * pairs - tile)
            lanes = slice(tile * LANES, (tile + count) * LANES)
            packed = jnp.dot(tokens, weight[:, lanes], preferred_element_type=jnp.float32) + bias[side:side + 1, lanes]
            for k in range(count):
                kind, p = (tile + k) // pairs, (tile + k) % pairs
                value = packed[:, k * LANES:(k + 1) * LANES]
                if kind < 2:
                    value = unit(value, gain[side:side + 1, (tile + k) * LANES:(tile + k + 1) * LANES])
                else:
                    value = value.T.astype(jnp.bfloat16)
                offset = 0
                for start, size in spans:
                    if kind == 0:
                        q_s[p, pl.ds(start, size), :] = value[offset:offset + size]
                    elif kind == 1:
                        k_s[p, pl.ds(start, size), :] = value[offset:offset + size]
                    else:
                        v_s[p, :, pl.ds(start, size)] = value[:, offset:offset + size]
                    offset += size

    for copy in weights:
        copy.wait()
    half_rows = rows // 2

    @pl.loop(0, n)
    def _(step):
        @pl.when(step == 1)
        def _():
            forward(0, lside, 0, right)
            forward(1, rside, 2, left)
            forward(0, lside, 4, right)
            forward(0, lside, 1, right)
            forward(1, rside, 3, left)

        @pl.when(step == 2)
        def _():
            for q in (2, 3):
                arrived(0, lside, q)
            for q in (4, 0, 1):
                arrived(1, rside, q)

        @pl.when(step == 3)
        def _():
            for q in (4, 0, 2, 1, 3):
                arrived(2, far, q)

        shift = (3 * step + 3 * (step // 2) + 2 * (step // 3)) % n
        one, two = (me + shift) % n, (me + n - shift) % n
        tokens = jnp.concatenate([a_img[one, :half_rows, :], a_img[two, half_rows:, :]], axis=0)
        project(tokens, w_i, 0, ((pl.multiple_of(one * rows, half_rows), half_rows), (pl.multiple_of(two * rows + half_rows, half_rows), half_rows)))

    fill = jnp.zeros((all_rows - img_rows - n * txt_rows, width), txt.dtype)
    project(jnp.concatenate([a_txt[...].reshape(n * txt_rows, width), fill], axis=0), w_t, 1, ((img_rows, all_rows - img_rows),))

    factor = math.log2(math.e) / math.sqrt(head_dim)
    chunks = all_rows // K_BLOCK
    blocks = all_rows // Q_BLOCK

    def query(index, h):
        value = q_s[index // blocks, pl.ds(pl.multiple_of((index % blocks) * Q_BLOCK, Q_BLOCK), Q_BLOCK), :]
        zero = jnp.zeros_like(value)
        return jnp.where(low, value, zero) if h == 0 else jnp.where(low, zero, value)

    def fold(tile):
        return tile.reshape(tile.shape[0] // 8, 8, tile.shape[1])

    def score(index, value, s_ref, ch, top):
        span = slice(ch * K_BLOCK, (ch + 1) * K_BLOCK)
        tile = lax.dot_general(k_s[index // blocks, span, :], value, (((1,), (1,)), ((), ())), preferred_element_type=jnp.float32)
        if ch == chunks - 1:
            tile = tile + jnp.concatenate([key_bias[...]] * (Q_BLOCK // LANES), axis=1)
        s_ref[span, :] = tile
        peak = jnp.max(fold(tile), axis=0)
        return peak if top is None else jnp.maximum(top, peak)

    def weigh(index, h, s_ref, ch, top, norm, out):
        span = slice(ch * K_BLOCK, (ch + 1) * K_BLOCK)
        prob = jnp.exp2((s_ref[span, :] - top) * factor)
        norm = norm + jnp.sum(fold(prob), axis=0)
        out = out + jnp.dot(v_s[index // blocks, h * head_dim:(h + 1) * head_dim, span], prob.astype(jnp.bfloat16), preferred_element_type=jnp.float32)
        return norm, out

    def stage(next_index, next_h, s_next, index, h, s_now, top_now):
        top = None
        value = query(next_index, next_h)
        norm = jnp.zeros((8, Q_BLOCK), jnp.float32)
        out = jnp.zeros((head_dim, Q_BLOCK), jnp.float32)
        for ch in range(chunks):
            top = score(next_index, value, s_next, ch, top)
            norm, out = weigh(index, h, s_now, ch, top_now, norm, out)
        return jnp.max(top, axis=0, keepdims=True), out / jnp.sum(norm, axis=0, keepdims=True)

    def o_copies(p, d, owner):
        member = (me + d) % n
        lanes = pl.ds(pl.multiple_of(owner * cols + p * LANES, LANES), LANES)
        sources = (o_s.at[p, pl.ds(pl.multiple_of(member * rows, rows), rows)], o_s.at[p, pl.ds(pl.multiple_of(img_rows + member * txt_rows, 16), txt_rows)])
        return list(zip(sources, (img_o.at[:, lanes], txt_o.at[:, lanes])))

    def o_remote(p, d, owner):
        return [remote(src, dst, o_send.at[p, d, t], o_recv.at[p, d, t], *peer(d)) for t, (src, dst) in enumerate(o_copies(p, d, owner))]

    top = None
    value = query(0, 0)
    for ch in range(chunks):
        top = score(0, value, s_a, ch, top)
    top = jnp.max(top, axis=0, keepdims=True)
    steps = pairs * blocks

    def body(step, top_a):
        after = (step + 1) % steps
        top_b, out_a = stage(step, 1, s_b, step, 0, s_a, top_a)
        top_a, out_b = stage(after, 0, s_a, step, 1, s_b, top_b)
        p, b = step // blocks, step % blocks
        o_s[p, pl.ds(pl.multiple_of(b * Q_BLOCK, Q_BLOCK), Q_BLOCK), :] = jnp.concatenate([out_a, out_b], axis=0).T.astype(jnp.bfloat16)

        @pl.when(b == blocks - 1)
        def _():
            for d in (2, 1, 3):
                for copy in o_remote(p, d, me):
                    copy.start()
            for t, (src, dst) in enumerate(o_copies(p, 0, me)):
                pltpu.make_async_copy(src, dst, o_send.at[p, 0, t]).start()

        return top_a

    lax.fori_loop(0, steps, body, top)
    for copy in copies:
        copy.wait_send()
    for kind, slot, q, target in ((0, lside, 0, right), (1, rside, 2, left), (0, lside, 1, right), (1, rside, 3, left), (0, lside, 4, right)):
        remote(landing(slot, q), landing(slot, q), send.at[2, q], recv.at[2, q], *target).wait_send()
    for p in range(pairs):
        for t, (src, dst) in enumerate(o_copies(p, 0, me)):
            pltpu.make_async_copy(src, dst, o_send.at[p, 0, t]).wait()
        for d in range(1, n):
            for copy in o_remote(p, d, me):
                copy.wait_send()
            for copy in o_remote(p, d, (me + n - d) % n):
                copy.wait_recv()


def joint(mesh, img, txt, mod, w_qkv, b_qkv, gains, valid, txt_run, block, head_dim, collective_id):
    n = mesh.shape['u']
    width = img.shape[1]
    all_rows = n * img.shape[0] + TXT_ROWS
    cols = width // n
    pairs = cols // LANES
    bf16, f32 = jnp.bfloat16, jnp.float32
    vmem = pl.BlockSpec(memory_space=VMEM)
    return pl.pallas_call(
        functools.partial(joint_kernel, n, head_dim, txt_run, block),
        out_shape=[jax.ShapeDtypeStruct(img.shape, bf16), jax.ShapeDtypeStruct(txt.shape, bf16)],
        in_specs=[vmem, vmem, vmem, pl.BlockSpec(memory_space=pl.ANY), vmem, vmem, vmem, vmem],
        out_specs=[vmem, vmem],
        scratch_shapes=[
            pltpu.VMEM((2, 3 * cols), f32), pltpu.VMEM((2, 2 * cols), f32), pltpu.VMEM((TXT_ROWS, LANES), f32),
            pltpu.VMEM((n,) + img.shape, bf16), pltpu.VMEM((n,) + txt.shape, bf16),
            pltpu.VMEM((width, 3 * cols), bf16), pltpu.VMEM((width, 3 * cols), bf16),
            pltpu.VMEM((pairs, all_rows, LANES), bf16), pltpu.VMEM((pairs, all_rows, LANES), bf16), pltpu.VMEM((pairs, LANES, all_rows), bf16),
            pltpu.VMEM((all_rows, Q_BLOCK), f32), pltpu.VMEM((all_rows, Q_BLOCK), f32),
            pltpu.VMEM((pairs, all_rows, LANES), bf16),
            pltpu.SemaphoreType.DMA((3, 5)), pltpu.SemaphoreType.DMA((3, 5)),
            pltpu.SemaphoreType.DMA((pairs, n, 2)), pltpu.SemaphoreType.DMA((pairs, n, 2)),
            pltpu.SemaphoreType.DMA((8,)),
        ],
        compiler_params=pltpu.CompilerParams(collective_id=collective_id, has_side_effects=True, vmem_limit_bytes=60 * 2**20),
        cost_estimate=pl.CostEstimate(flops=4 * 10**10, bytes_accessed=10**7, transcendentals=0),
        name='joint',
    )(img, txt, mod, w_qkv, b_qkv, *gains, valid)


def mlp_kernel(x_i, x_t, o_i, o_t, mod, wp_i, wp_t, wu_i, wu_t, wd_i, wd_t, b_proj, b_down, b_up, y_i, y_t, r_i, r_t, a_i, a_t, acc_i, acc_t):
    outs = (y_i, y_t)
    step = pl.program_id(0)
    tiles = pl.num_programs(0)
    sides = ((x_i, o_i, wp_i, wu_i, wd_i, b_up, r_i, a_i, acc_i), (x_t, o_t, wp_t, wu_t, wd_t, b_up, r_t, a_t, acc_t))

    def both(ref):
        return ref[0].astype(jnp.float32)

    def row(ref, side, k):
        return ref[side, k:k + 1, :]

    def row_blocks(ref):
        size = min(ref.shape[0], ROW_BLOCK)
        return [pl.ds(start, size) for start in range(0, ref.shape[0], size)]

    @pl.when(step == 0)
    def _():
        for side, (x, o, wp, wu, wd, bu, r, a, acc) in enumerate(sides):
            for span in row_blocks(x):
                lin = jnp.dot(o[span, :], wp[0, 0], preferred_element_type=jnp.float32) + both(b_proj)[side:side + 1]
                hidden = (x[span, :].astype(jnp.float32) + row(mod, side, 2) * lin).astype(jnp.bfloat16)
                r[span, :] = hidden
                a[span, :] = modulated_norm(hidden, row(mod, side, 3), row(mod, side, 4))
                acc[span, :] = jnp.zeros_like(acc[span, :])

    for side, (x, o, wp, wu, wd, bu, r, a, acc) in enumerate(sides):
        for span in row_blocks(x):
            inner = jnp.dot(a[span, :], wu[0, 0], preferred_element_type=jnp.float32) + both(bu)[side:side + 1]
            inner = jax.nn.gelu(inner, approximate=True).astype(jnp.bfloat16)
            acc[span, :] += jnp.dot(inner, wd[0, 0], preferred_element_type=jnp.float32)

    @pl.when(step == tiles - 1)
    def _():
        for side, (x, o, wp, wu, wd, bu, r, a, acc) in enumerate(sides):
            for span in row_blocks(x):
                lin = acc[span, :] + both(b_down)[side:side + 1]
                hidden = (r[span, :].astype(jnp.float32) + row(mod, side, 5) * lin).astype(jnp.bfloat16)
                outs[side][span, :] = hidden


def mlp(sides, attended, mod, w_proj, b_proj, w_up, b_up, w_down, b_down, block):
    width, inner = w_up.shape[2:]
    tiles = inner // MLP_TILE
    whole = lambda shape: pl.BlockSpec(shape, lambda t: (0,) * len(shape))
    sizes = [sides[0].shape, sides[1].shape]
    wp = [pl.BlockSpec((1, 1, width, width), lambda t, s=s: (block, s, 0, 0)) for s in range(2)]
    wu = [pl.BlockSpec((1, 1, width, MLP_TILE), lambda t, s=s: (block, s, 0, t)) for s in range(2)]
    wd = [pl.BlockSpec((1, 1, MLP_TILE, width), lambda t, s=s: (block, s, t, 0)) for s in range(2)]
    rows = pl.BlockSpec((1, 2, width), lambda t: (block, 0, 0))
    bu = pl.BlockSpec((1, 2, MLP_TILE), lambda t: (block, 0, t))
    shapes = [jax.ShapeDtypeStruct(size, jnp.bfloat16) for size in sizes]
    scratch = [pltpu.VMEM(size, dtype) for dtype in (jnp.bfloat16, jnp.bfloat16, jnp.float32) for size in sizes]
    return pl.pallas_call(
        mlp_kernel,
        out_shape=shapes,
        grid=(tiles,),
        in_specs=[whole(s) for s in sizes] * 2 + [whole(mod.shape)] + wp + wu + wd + [rows, rows, bu],
        out_specs=[whole(s.shape) for s in shapes],
        scratch_shapes=scratch,
        compiler_params=pltpu.CompilerParams(vmem_limit_bytes=60 * 2**20, dimension_semantics=('arbitrary',)),
        cost_estimate=pl.CostEstimate(flops=25 * 10**9, bytes_accessed=86 * 10**6, transcendentals=0),
        name='mlp',
    )(sides[0], sides[1], attended[0], attended[1], mod, w_proj, w_proj, w_up, w_up, w_down, w_down, b_proj, b_down, b_up)


def solution(mesh):
    seq_spec = P('dp', ('r', 'u'), None)
    row_spec = P('dp', None)
    n = mesh.shape['u']

    def local_blocks(image, text, cond_vec, key_valid, w_mod, b_mod, w_qkv, b_qkv, q_gain, k_gain, w_proj, b_proj, w_up, b_up, w_down, b_down):
        blocks, _, width, _ = w_mod.shape
        head_dim = q_gain.shape[3]
        img, txt, mod_all = scatter(mesh, image, text, cond_vec, w_mod, b_mod)
        mod_all = mod_all.reshape(blocks, 2, 6, width)
        slots, run, _ = img.shape
        txt_run = txt.shape[1]
        img = img.reshape(slots * run, width)
        txt = jnp.pad(txt.reshape(slots * txt_run, width), ((0, TXT_PAD - slots * txt_run), (0, 0)))

        gains = [gain.reshape(blocks, 2, width) for gain in (q_gain, k_gain)]
        valid = key_valid.astype(jnp.float32)

        sides = [img, txt]
        for block in range(blocks):
            attended = joint(mesh, sides[0], sides[1], mod_all[block], w_qkv, b_qkv, gains, valid, txt_run, block, head_dim, 2 + block)
            sides = mlp(sides, attended, mod_all[block], w_proj, b_proj, w_up, b_up, w_down, b_down, block)
        img = sides[0].reshape(slots, run, width)
        txt = sides[1][: slots * txt_run].reshape(slots, txt_run, width)
        return unscatter(mesh, img, txt)

    return jax.shard_map(local_blocks, mesh=mesh, in_specs=(seq_spec, seq_spec, row_spec, row_spec) + (P(),) * 12, out_specs=(seq_spec, seq_spec), check_vma=False)
```
